32 devices in a mesh: section: 8 (over y, x, core), tensor: 4 (over z).
Axes of the slice: x: 2, y: 2, z: 4, core: 2. Of those that a mesh axis runs over, the one named last changes fastest.
Arguments:
- arriving: bfloat16 [8, 512, 16384], P('section', 'tensor'), may hold values from -6 to 6
- kept_input: bfloat16 [8, 512, 16384], P('section', 'tensor'), may hold values from -6 to 6
- returning: bfloat16 [8, 512, 16384], P('section', 'tensor'), may hold values from -6 to 6
- norm_gain: bfloat16 [8, 16384], P('section'), may hold values from 0.25 to 1.75
- key_weight: bfloat16 [8, 16384, 1024], P('section', 'tensor'), may hold values from -0.0625 to 0.0625
- value_weight: bfloat16 [8, 16384, 1024], P('section', 'tensor'), may hold values from -0.0625 to 0.0625
- key_down: bfloat16 [8, 16384, 16], P('section', 'tensor'), may hold values from -0.046875 to 0.046875
- value_down: bfloat16 [8, 16384, 16], P('section', 'tensor'), may hold values from -0.046875 to 0.046875
- key_up: bfloat16 [8, 16, 1024], P('section', None, 'tensor'), may hold values from -1.5 to 1.5
- value_up: bfloat16 [8, 16, 1024], P('section', None, 'tensor'), may hold values from -1.5 to 1.5
- key_cot: bfloat16 [8, 512, 1024], P('section', None, 'tensor'), may hold values from -6 to 6
- value_cot: bfloat16 [8, 512, 1024], P('section', None, 'tensor'), may hold values from -6 to 6
Outputs:
- keys: bfloat16 [8, 512, 1024], P('section', None, 'tensor')
- values: bfloat16 [8, 512, 1024], P('section', None, 'tensor')
- input_grad: bfloat16 [8, 512, 16384], P('section', 'tensor')
- key_down_grad: float32 [8, 16384, 16], P('section', 'tensor')
- value_down_grad: float32 [8, 16384, 16], P('section', 'tensor')
- key_up_grad: float32 [8, 16, 1024], P('section', None, 'tensor')
- value_up_grad: float32 [8, 16, 1024], P('section', None, 'tensor')
The draws below stay inside these ranges and needn't reach their ends.
All inputs are finite; a program needn't handle non-finite values.
Results may differ from the reference program's by a relative error of at most 0.014.
Values may be sent and summed in bfloat16 or wider, within the bound.
A program may use at most 192 MiB of HBM per device.

```python
import jax
import jax.numpy as jnp
from jax import lax

D = 16384
RANK = 16
TOKENS = 512
KVW = 1024
LAYERS = 8


def with_spikes(values, stream_key, source, target, blocks, factor):
    def block_of(position):
        return (jnp.arange(values.shape[position]) // (values.shape[position] // blocks)).reshape((-1,) + (1,) * (values.ndim - 1 - position))

    one_side = jax.random.permutation(stream_key, blocks)[block_of(target)]
    other_side = (block_of(target) + blocks // 2) % blocks
    return jnp.where((block_of(source) == one_side) | (block_of(source) == other_side), factor * values, values)


def block_scale(stream_key, dims, cuts, low, high):
    level = 1.0
    for position, shards_of in cuts:
        draws = jax.random.uniform(jax.random.fold_in(jax.random.fold_in(stream_key, 6), position), (shards_of,), jnp.float32, low / len(cuts), high / len(cuts))
        level = level * jnp.repeat(jnp.exp(draws), dims[position] // shards_of).reshape((-1,) + (1,) * (len(dims) - 1 - position))
    return level


def bell_draw(key, extent, scale, reach, shards=(), held_as=jnp.bfloat16):
    factor_of = block_scale(key, extent, shards, -0.22, 0.18) if shards else 1.0
    result = jax.random.normal(key, extent, jnp.float32) * scale * factor_of
    return jnp.minimum(jnp.maximum(result, -reach), reach).astype(held_as)


def noise_with(stream_key, extent, spread, bound, pieces, heavy, dtype=jnp.bfloat16):
    entries = spread * jax.random.normal(stream_key, extent, jnp.float32)
    if pieces:
        entries = entries * block_scale(stream_key, extent, pieces, -0.22, 0.18)
    return jnp.clip(with_spikes(entries, jax.random.fold_in(stream_key, 3), *heavy), -bound, bound).astype(dtype)


def setup_inputs(seed: int = 0) -> dict:
    key_of = jax.random.split(jax.random.key(seed), 13)
    return {
        "arriving": bell_draw(key_of[0], (LAYERS, TOKENS, D), 1.0, 6.0, ((0, 8), (1, 4))),
        "kept_input": bell_draw(key_of[1], (LAYERS, TOKENS, D), 1.0, 6.0, ((0, 8), (1, 4))),
        "returning": bell_draw(key_of[2], (LAYERS, TOKENS, D), 1.0, 6.0, ((0, 8), (1, 4))),
        "norm_gain": jnp.clip(1.0 + 0.15 * jax.random.normal(key_of[3], (LAYERS, D), jnp.float32), 0.25, 1.75).astype(jnp.bfloat16),
        "key_weight": noise_with(key_of[4], (LAYERS, D, KVW), D ** -0.5, 0.0625, ((0, 8), (1, 4)), (1, 2, 4, 2.0)),
        "value_weight": noise_with(key_of[5], (LAYERS, D, KVW), D ** -0.5, 0.0625, ((0, 8), (1, 4)), (1, 2, 4, 2.0)),
        "key_down": bell_draw(key_of[6], (LAYERS, D, RANK), D ** -0.5, 0.046875, ((0, 8), (1, 4))),
        "value_down": bell_draw(key_of[7], (LAYERS, D, RANK), D ** -0.5, 0.046875, ((0, 8), (1, 4))),
        "key_up": bell_draw(key_of[8], (LAYERS, RANK, KVW), RANK ** -0.5, 1.5, ((0, 8), (2, 4))),
        "value_up": bell_draw(key_of[9], (LAYERS, RANK, KVW), RANK ** -0.5, 1.5, ((0, 8), (2, 4))),
        "key_cot": bell_draw(key_of[10], (LAYERS, TOKENS, KVW), 1.0, 6.0, ((0, 8), (2, 4))),
        "value_cot": bell_draw(key_of[11], (LAYERS, TOKENS, KVW), 1.0, 6.0, ((0, 8), (2, 4))),
    }


epsilon = 1e-05
adapter_scale = 2.0

def normalize(hidden, gain):
    values = hidden.astype(jnp.float32)
    inverse = lax.rsqrt(lax.optimization_barrier(jnp.mean(values * values, axis=-1, keepdims=True)) + epsilon)
    return (inverse, (values * inverse * gain.astype(jnp.float32)).astype(jnp.bfloat16))

def precise_product(left, right):
    return jnp.dot(left, right, precision=lax.Precision.HIGHEST, preferred_element_type=jnp.float32)

def mixed_product(left, right):
    return jnp.dot(left.astype(jnp.float32), right.astype(jnp.float32), preferred_element_type=jnp.float32)

def one_layer(blocks):
    incoming, kept, back, gain, key_matrix, value_matrix, key_down_matrix, value_down_matrix, key_up_matrix, value_up_matrix, key_cotangent, value_cotangent = blocks
    _, normed_input = normalize(incoming, gain)
    key_middle = mixed_product(normed_input, key_down_matrix)
    value_middle = mixed_product(normed_input, value_down_matrix)
    keys = (mixed_product(normed_input, key_matrix) + adapter_scale * precise_product(key_middle, key_up_matrix.astype(jnp.float32))).astype(jnp.bfloat16)
    values = (mixed_product(normed_input, value_matrix) + adapter_scale * precise_product(value_middle, value_up_matrix.astype(jnp.float32))).astype(jnp.bfloat16)
    adapted_key = mixed_product(key_cotangent, key_up_matrix.T)
    adapted_value = mixed_product(value_cotangent, value_up_matrix.T)
    branch_output = mixed_product(key_cotangent, key_matrix.T) + mixed_product(value_cotangent, value_matrix.T)
    branch_output = branch_output + adapter_scale * (precise_product(adapted_key, key_down_matrix.T.astype(jnp.float32)) + precise_product(adapted_value, value_down_matrix.T.astype(jnp.float32)))
    branch_output = lax.optimization_barrier(branch_output.astype(jnp.bfloat16)).astype(jnp.float32)
    inverse, kept_normed = normalize(kept, gain)
    kept_values = kept.astype(jnp.float32)
    scaled = gain.astype(jnp.float32) * branch_output
    inner = lax.optimization_barrier(jnp.mean(kept_values * scaled, axis=-1, keepdims=True))
    input_grad = (back.astype(jnp.float32) + inverse * scaled - kept_values * inverse * inverse * inverse * inner).astype(jnp.bfloat16)
    saved_wide_input = kept_normed.astype(jnp.float32)
    key_down_gradient = adapter_scale * precise_product(saved_wide_input.T, adapted_key)
    value_down_gradient = adapter_scale * precise_product(saved_wide_input.T, adapted_value)
    key_middle_rows = mixed_product(kept_normed, key_down_matrix)
    value_middle_rows = mixed_product(kept_normed, value_down_matrix)
    key_up_gradient = adapter_scale * precise_product(key_middle_rows.T, key_cotangent.astype(jnp.float32))
    value_up_gradient = adapter_scale * precise_product(value_middle_rows.T, value_cotangent.astype(jnp.float32))
    return (keys, values, input_grad, key_down_gradient, value_down_gradient, key_up_gradient, value_up_gradient)

def reference(arriving, kept_input, returning, norm_gain, key_weight, value_weight, key_down, value_down, key_up, value_up, key_cot, value_cot):
    incoming = jnp.roll(arriving, 1, axis=0)
    back = jnp.roll(returning, -1, axis=0)
    layer_count = arriving.shape[0]
    collected = []
    for layer in range(layer_count):
        blocks = (incoming[layer], kept_input[layer], back[layer], norm_gain[layer], key_weight[layer], value_weight[layer], key_down[layer], value_down[layer], key_up[layer], value_up[layer], key_cot[layer], value_cot[layer])
        collected.append(one_layer(blocks))
    stacked = [jnp.stack([item[index] for item in collected], axis=0) for index in range(7)]
    return (stacked[0], stacked[1], stacked[2], stacked[3], stacked[4], stacked[5], stacked[6])
```

```python
import functools

import jax
import jax.numpy as jnp
from jax import lax
from jax.experimental import pallas as pl
from jax.experimental.pallas import tpu as pltpu
from jax.sharding import PartitionSpec as P

epsilon = 1e-05
adapter_scale = 2.0
bf16 = jnp.bfloat16
f32 = jnp.float32
MESH = pl.DeviceIdType.MESH
lanes = 128
parts = 4
halves = 2
row_tile = 16


def flip(z, mask):
    bit = 1
    while bit <= mask:
        if mask & bit:
            z = z + bit - 2 * bit * ((z // bit) % 2)
        bit *= 2
    return z


def bits_up(count):
    bits = []
    bit = 1
    while bit < count:
        bits.append(bit)
        bit *= 2
    return bits


def dot_nt(a, b):
    return lax.dot_general(a, b, (((1,), (1,)), ((), ())), preferred_element_type=f32)


def dot_nn(a, b):
    return jnp.dot(a, b, preferred_element_type=f32)


def layer_kernel(
    count,
    sections,
    gain_ref,
    arr,
    kept,
    ret,
    wk,
    wv,
    dnk,
    dnv,
    upk,
    upv,
    ck,
    cv,
    keys_out,
    values_out,
    grad_out,
    dgk_out,
    dgv_out,
    ugk_out,
    ugv_out,
    wk_v,
    wv_v,
    cotk,
    cotv,
    upk_v,
    upv_v,
    dn_v,
    arr_v,
    kept_v,
    back_v,
    x_v,
    inv_t,
    inv_in,
    inv_f,
    inv_b,
    ad_v,
    adt_v,
    mid_v,
    bo_v,
    bi_v,
    nb_v,
    dp_v,
    dp_in,
    km_v,
    sums_v,
    sums_in,
    kv_v,
    dg_v,
    ug_v,
    send_sem,
    recv_sem,
    local_sem,
):
    rows, width = kept.shape
    depth = wk.shape[0]
    tokens, heads = ck.shape
    rank = upk.shape[0]
    s = lax.axis_index("section")
    z = lax.axis_index("tensor")
    ahead = lax.rem(s + 1, sections)
    behind = lax.rem(s + sections - 1, sections)
    used = [0, 0]

    def load(src, dst):
        copy = pltpu.make_async_copy(src, dst, local_sem.at[used[1]])
        used[1] += 1
        copy.start()
        return copy

    sent = []

    def send(src, dst, section, tensor):
        k = used[0]
        used[0] += 1
        copy = pltpu.make_async_remote_copy(
            src_ref=src,
            dst_ref=dst,
            send_sem=send_sem.at[k],
            recv_sem=recv_sem.at[k],
            device_id=(section, tensor),
            device_id_type=MESH,
        )
        copy.start()
        sent.append(copy)
        return copy

    def head_cols(q):
        return pl.ds(pl.multiple_of(q * heads, heads), heads)

    def depth_cols(q):
        return pl.ds(pl.multiple_of(q * depth, depth), depth)

    bits = bits_up(count)
    down_bits = list(reversed(bits))
    own = [
        load(ck, cotk.at[:, head_cols(z)]),
        load(cv, cotv.at[:, head_cols(z)]),
        load(upk, upk_v.at[:, head_cols(z)]),
        load(upv, upv_v.at[:, head_cols(z)]),
    ]
    own_down = [load(dnk, dn_v.at[z, :rank]), load(dnv, dn_v.at[z, rank:])]
    arr_load = load(arr, arr_v)
    kept_load = load(kept, kept_v)
    weights = [load(wk, wk_v), load(wv, wv_v)]

    def gather_stage(held, bit, kinds):
        to = flip(z, bit)
        copies = []
        for h in held:
            q = flip(z, h)
            if "c" in kinds:
                for src, dst in ((ck, cotk), (cv, cotv), (upk, upk_v), (upv, upv_v)):
                    block = dst.at[:, head_cols(q)]
                    copies.append(send(block if h else src, block, s, to))
            if "d" in kinds:
                copies.append(send(dn_v.at[q], dn_v.at[q], s, to))
        return copies

    half = rows // halves

    def send_arriving(j, i):
        q = flip(z, j)
        at = pl.ds(i * half, half)
        return send(arr.at[at, depth_cols(q)], x_v.at[z, at], ahead, q)

    far = [j for j in range(count) if j >= max(bits[-1], 1)] if bits else []
    near = [j for j in range(1, count) if j not in far]
    arrivals = {}
    held = [0]
    stage = gather_stage(held, down_bits[0], "c") if bits else []
    for i in range(halves):
        arrivals[0, i] = send_arriving(0, i)
    for j in far:
        arrivals[j, 0] = send_arriving(j, 0)
    returned = send(ret, back_v, behind, z)
    for copy in own_down:
        copy.wait()
    down_stage = gather_stage(held, down_bits[0], "d") if bits else []

    arr_load.wait()

    def arr_stats(i, _):
        at = pl.ds(pl.multiple_of(i * row_tile, row_tile), row_tile)
        x = arr_v[at, :].astype(f32)
        inverse = lax.rsqrt(jnp.mean(x * x, axis=-1, keepdims=True) + epsilon)
        inv_t[at, :] = jnp.broadcast_to(inverse, (row_tile, lanes))
        return 0

    lax.fori_loop(0, rows // row_tile, arr_stats, 0)
    inv_in[z] = inv_t[...].T[:8]
    inverses = [send(inv_in.at[z], inv_in.at[z + count], ahead, flip(z, j)) for j in range(count)]
    kept_load.wait()

    def kept_stats(i, _):
        at = pl.ds(pl.multiple_of(i * row_tile, row_tile), row_tile)
        x = kept_v[at, :].astype(f32)
        inverse = lax.rsqrt(jnp.mean(x * x, axis=-1, keepdims=True) + epsilon)
        inv_b[at, :] = jnp.broadcast_to(inverse, (row_tile, lanes))
        return 0

    lax.fori_loop(0, rows // row_tile, kept_stats, 0)

    for bit in down_bits[:1]:
        for copy in stage:
            copy.wait_recv()
        held = held + [h ^ bit for h in held]
    waiting = list(down_stage)
    for bit in down_bits[1:]:
        stage = gather_stage(held, bit, "c")
        if bit == down_bits[1]:
            for i in range(1, halves):
                for j in far:
                    arrivals[j, i] = send_arriving(j, i)
        for copy in waiting:
            copy.wait_recv()
        waiting = gather_stage(held, bit, "d")
        for copy in stage:
            copy.wait_recv()
        held = held + [h ^ bit for h in held]
    for i in range(halves):
        for j in near + far:
            if (j, i) not in arrivals:
                arrivals[j, i] = send_arriving(j, i)
    for copy in own + weights:
        copy.wait()

    for r, (cot, up) in enumerate(((cotk, upk_v), (cotv, upv_v))):
        ad_v[:, r * rank : (r + 1) * rank] = adapter_scale * dot_nt(cot[...], up[...])
        adt_v[r * rank : (r + 1) * rank, :] = adapter_scale * dot_nt(up[...], cot[...])

    tile = min(512, depth)

    def branch_tile(i, _):
        at = pl.ds(pl.multiple_of(i * tile, tile), tile)
        total = dot_nn(ad_v[...].astype(bf16), dn_v[z, :, at])
        total = total + dot_nt(cotk[...], wk_v[at, :])
        total = total + dot_nt(cotv[...], wv_v[at, :])
        bo_v[:, :, at] = total.astype(bf16).reshape(count, rows, tile)
        return 0

    lax.fori_loop(0, depth // tile, branch_tile, 0)
    part = rows // parts
    others = far + near
    branches = {}

    def send_branch(i):
        at = pl.ds(i * part, part)
        for j in others:
            q = flip(z, j)
            branches[j, i] = send(bo_v.at[q, at], bi_v.at[z, at], s, q)

    for i in range(parts // 2):
        send_branch(i)

    def own_branch(i, _):
        at = pl.ds(pl.multiple_of(i * row_tile, row_tile), row_tile)
        bi_v[z, at, :] = bo_v[z, at, :]
        return 0

    lax.fori_loop(0, rows // row_tile, own_branch, 0)

    for copy in waiting:
        copy.wait_recv()
    mine = adt_v[:, pl.ds(pl.multiple_of(z * rows, rows), rows)].astype(bf16)

    km_v[z] = jnp.zeros((2 * rank, rows), f32)

    def kept_block(j, _):
        inverse = inv_b[:, :1]

        def normalize(i, _):
            at = pl.ds(pl.multiple_of(i * tile, tile), tile)
            cols = pl.ds(pl.multiple_of(j * depth + i * tile, tile), tile)
            part = kept_v[:, cols].astype(f32) * inverse * gain_ref[:, cols].astype(f32)
            nb_v[:, at] = part.astype(bf16)
            return 0

        lax.fori_loop(0, depth // tile, normalize, 0)
        km_v[z] += dot_nt(dn_v[j], nb_v[...])
        dp_v[j] = dot_nn(mine, nb_v[...]).astype(bf16)
        return 0

    lax.fori_loop(0, count, kept_block, 0)
    mids = [send(km_v.at[z], km_v.at[z], s, flip(z, j)) for j in range(1, count)]

    def scatter_stage(buf, landing, bit):
        to = flip(z, bit)
        offset = sum(count // (2 * b) for b in bits if b < bit)
        return [
            send(buf.at[flip(z, bit ^ m)], landing.at[offset + k], s, to)
            for k, m in enumerate(range(0, count, 2 * bit))
        ]

    def scatter_add(buf, landing, bit, copies):
        offset = sum(count // (2 * b) for b in bits if b < bit)
        for k, m in enumerate(range(0, count, 2 * bit)):
            copies[k].wait_recv()
            q = flip(z, m)
            buf[q] = (buf[q].astype(f32) + landing[offset + k].astype(f32)).astype(bf16)

    stores = []
    down_stage = scatter_stage(dp_v, dp_in, bits[0]) if bits else []

    def head_block(q):
        gain_cols = depth_cols(z)

        def scale(i, _):
            at = pl.ds(pl.multiple_of(i * row_tile, row_tile), row_tile)
            x_v[q, at, :] = (x_v[q, at, :].astype(f32) * gain_ref[:, gain_cols].astype(f32)).astype(bf16)
            return 0

        lax.fori_loop(0, rows // row_tile, scale, 0)
        mid = adapter_scale * dot_nt(x_v[q], dn_v[z])
        mid_v[...] = mid.astype(bf16)
        at = pl.ds(pl.multiple_of(q * rows, rows), rows)

        def head_cut(d, _):
            cols = head_cols(d)
            for r, (w, up) in enumerate(((wk_v, upk_v), (wv_v, upv_v))):
                total = dot_nn(x_v[q], w[:, cols])
                total = total + dot_nn(mid_v[:, r * rank : (r + 1) * rank], up[:, cols])
                sums_v[d, r, at, :] = total.astype(bf16)
            return 0

        lax.fori_loop(0, count, head_cut, 0)

    for j in [0] + far + near:
        for i in range(halves):
            arrivals[j, i].wait_recv()
        head_block(flip(z, j))
    for k, bit in enumerate(bits):
        stage = scatter_stage(sums_v, sums_in, bit)
        if k == 0:
            send_branch(parts // 2)
        scatter_add(dp_v, dp_in, bit, down_stage)
        if k + 1 < len(bits):
            down_stage = scatter_stage(dp_v, dp_in, bits[k + 1])
        if k + 1 < len(bits):
            scatter_add(sums_v, sums_in, bit, stage)
    for i in range(parts // 2 + 1, parts):
        send_branch(i)

    dg_v[...] = dp_v[z].astype(f32)
    stores.append(load(dg_v.at[:rank], dgk_out))
    stores.append(load(dg_v.at[rank:], dgv_out))
    for copy in mids:
        copy.wait_recv()
    for r, cot in enumerate((cotk, cotv)):
        total = jnp.zeros((rank, heads), f32)
        for q in range(count):
            mid = (adapter_scale * km_v[q, r * rank : (r + 1) * rank, :]).astype(bf16)
            total = total + dot_nn(mid, cot[q * rows : (q + 1) * rows, head_cols(z)])
        ug_v[r] = total
    stores.append(load(ug_v.at[0], ugk_out))
    stores.append(load(ug_v.at[1], ugv_out))
    for copy in inverses:
        copy.wait_recv()
    for q in range(count):
        spread = jnp.broadcast_to(inv_in[count + q, :1, :], (lanes, rows)).T
        inv_f[q * rows : (q + 1) * rows, :] = spread
    returned.wait_recv()

    def grad_tile(i, _):
        at = pl.ds(pl.multiple_of(i * row_tile, row_tile), row_tile)
        inverse = inv_b[at, :1]
        inner = jnp.zeros((row_tile, 1), f32)
        for j in range(count):
            cols = slice(j * depth, (j + 1) * depth)
            scaled = gain_ref[:, cols].astype(f32) * bi_v[j, at, :].astype(f32)
            inner = inner + jnp.sum(kept_v[at, cols].astype(f32) * scaled, axis=-1, keepdims=True)
        pull = inverse * inverse * inverse * (inner / width)
        for j in range(count):
            cols = slice(j * depth, (j + 1) * depth)
            scaled = gain_ref[:, cols].astype(f32) * bi_v[j, at, :].astype(f32)
            value = back_v[at, cols].astype(f32) + inverse * scaled - kept_v[at, cols].astype(f32) * pull
            arr_v[at, cols] = value.astype(bf16)
        return 0

    def finish(i):
        for j in others:
            branches[j, i].wait_recv()
        lax.fori_loop(i * part // row_tile, (i + 1) * part // row_tile, grad_tile, 0)
        at = pl.ds(i * part, part)
        stores.append(load(arr_v.at[at], grad_out.at[at]))

    for i in range(parts - 1):
        finish(i)

    if bits:
        stage[0].wait_recv()

    def head_tile(i, _):
        at = pl.ds(pl.multiple_of(i * row_tile, row_tile), row_tile)
        for r in range(2):
            total = sums_v[z, r, at, :].astype(f32)
            if bits:
                total = total + sums_in[count - 2, r, at, :].astype(f32)
            kv_v[r, at, :] = (inv_f[at, :1] * total).astype(bf16)
        return 0

    lax.fori_loop(0, tokens // row_tile, head_tile, 0)
    stores.append(load(kv_v.at[0], keys_out))
    stores.append(load(kv_v.at[1], values_out))
    finish(parts - 1)
    for copy in sent:
        copy.wait_send()
    for copy in stores:
        copy.wait()


def run_layer(count, sections, arr, kept, ret, gain, wk, wv, dnk, dnv, upk, upv, ck, cv):
    rows, width = kept.shape
    depth, wide = wk.shape
    tokens, heads = ck.shape
    rank = upk.shape[0]
    copies = 4 * (count - 1) + (count - 1) + halves * count + count + 1
    copies += parts * (count - 1) + 3 * (count - 1)
    hbm = pl.BlockSpec(memory_space=pl.ANY)
    landing = max(count - 1, 1)
    return pl.pallas_call(
        functools.partial(layer_kernel, count, sections),
        in_specs=[pl.BlockSpec(memory_space=pltpu.VMEM)] + [hbm] * 11,
        out_specs=[hbm] * 7,
        out_shape=[
            jax.ShapeDtypeStruct((tokens, heads), bf16),
            jax.ShapeDtypeStruct((tokens, heads), bf16),
            jax.ShapeDtypeStruct((rows, width), bf16),
            jax.ShapeDtypeStruct((rank, depth), f32),
            jax.ShapeDtypeStruct((rank, depth), f32),
            jax.ShapeDtypeStruct((rank, heads), f32),
            jax.ShapeDtypeStruct((rank, heads), f32),
        ],
        scratch_shapes=[
            pltpu.VMEM((depth, wide), bf16),
            pltpu.VMEM((depth, wide), bf16),
            pltpu.VMEM((tokens, wide), bf16),
            pltpu.VMEM((tokens, wide), bf16),
            pltpu.VMEM((rank, wide), bf16),
            pltpu.VMEM((rank, wide), bf16),
            pltpu.VMEM((count, 2 * rank, depth), bf16),
            pltpu.VMEM((rows, width), bf16),
            pltpu.VMEM((rows, width), bf16),
            pltpu.VMEM((rows, width), bf16),
            pltpu.VMEM((count, rows, depth), bf16),
            pltpu.VMEM((rows, lanes), f32),
            pltpu.VMEM((2 * count, 8, rows), f32),
            pltpu.VMEM((tokens, lanes), f32),
            pltpu.VMEM((rows, lanes), f32),
            pltpu.VMEM((tokens, 2 * rank), f32),
            pltpu.VMEM((2 * rank, tokens), f32),
            pltpu.VMEM((rows, 2 * rank), bf16),
            pltpu.VMEM((count, rows, depth), bf16),
            pltpu.VMEM((count, rows, depth), bf16),
            pltpu.VMEM((rows, depth), bf16),
            pltpu.VMEM((count, 2 * rank, depth), bf16),
            pltpu.VMEM((landing, 2 * rank, depth), bf16),
            pltpu.VMEM((count, 2 * rank, rows), f32),
            pltpu.VMEM((count, 2, tokens, heads), bf16),
            pltpu.VMEM((landing, 2, tokens, heads), bf16),
            pltpu.VMEM((2, tokens, heads), bf16),
            pltpu.VMEM((2 * rank, depth), f32),
            pltpu.VMEM((2, rank, heads), f32),
            pltpu.SemaphoreType.DMA((copies,)),
            pltpu.SemaphoreType.DMA((copies,)),
            pltpu.SemaphoreType.DMA((10 + 6 + parts,)),
        ],
        compiler_params=pltpu.CompilerParams(
            has_side_effects=True, vmem_limit_bytes=67043328
        ),
        cost_estimate=pl.CostEstimate(
            flops=8 * tokens * depth * wide, bytes_accessed=4 * depth * wide, transcendentals=0
        ),
        name="layer",
    )(gain, arr, kept, ret, wk, wv, dnk, dnv, upk, upv, ck, cv)


def on_device(
    arriving,
    kept_input,
    returning,
    norm_gain,
    key_weight,
    value_weight,
    key_down,
    value_down,
    key_up,
    value_up,
    key_cot,
    value_cot,
):
    keys, values, input_grad, dgk, dgv, ugk, ugv = run_layer(
        lax.axis_size("tensor"),
        lax.axis_size("section"),
        arriving[0],
        kept_input[0],
        returning[0],
        norm_gain,
        key_weight[0],
        value_weight[0],
        key_down[0].T,
        value_down[0].T,
        key_up[0],
        value_up[0],
        key_cot[0],
        value_cot[0],
    )
    return (
        keys[None],
        values[None],
        input_grad[None],
        dgk.T[None],
        dgv.T[None],
        ugk[None],
        ugv[None],
    )


def solution(mesh):
    return jax.shard_map(
        on_device,
        mesh=mesh,
        in_specs=(
            P("section", "tensor", None),
            P("section", "tensor", None),
            P("section", "tensor", None),
            P("section", None),
            P("section", "tensor", None),
            P("section", "tensor", None),
            P("section", "tensor", None),
            P("section", "tensor", None),
            P("section", None, "tensor"),
            P("section", None, "tensor"),
            P("section", None, "tensor"),
            P("section", None, "tensor"),
        ),
        out_specs=(
            P("section", None, "tensor"),
            P("section", None, "tensor"),
            P("section", "tensor", None),
            P("section", "tensor", None),
            P("section", "tensor", None),
            P("section", None, "tensor"),
            P("section", None, "tensor"),
        ),
        check_vma=False,
    )
```

```python
import functools

import jax
import jax.numpy as jnp
from jax import lax
from jax.experimental import pallas as pl
from jax.experimental.pallas import tpu as pltpu
from jax.sharding import PartitionSpec as P

epsilon = 1e-05
adapter_scale = 2.0
bf16 = jnp.bfloat16
f32 = jnp.float32
MESH = pl.DeviceIdType.MESH
lanes = 128
parts = 4
halves = 2
row_tile = 16


def flip(z, mask):
    bit = 1
    while bit <= mask:
        if mask & bit:
            z = z + bit - 2 * bit * ((z // bit) % 2)
        bit *= 2
    return z


def bits_up(count):
    bits = []
    bit = 1
    while bit < count:
        bits.append(bit)
        bit *= 2
    return bits


def dot_nt(a, b):
    return lax.dot_general(a, b, (((1,), (1,)), ((), ())), preferred_element_type=f32)


def dot_nn(a, b):
    return jnp.dot(a, b, preferred_element_type=f32)


def layer_kernel(
    count,
    sections,
    gain_ref,
    arr,
    kept,
    ret,
    wk,
    wv,
    dnk,
    dnv,
    upk,
    upv,
    ck,
    cv,
    keys_out,
    values_out,
    grad_out,
    dgk_out,
    dgv_out,
    ugk_out,
    ugv_out,
    wk_v,
    wv_v,
    cotk,
    cotv,
    upk_v,
    upv_v,
    dn_v,
    arr_v,
    kept_v,
    back_v,
    x_v,
    inv_t,
    inv_in,
    inv_f,
    inv_b,
    ad_v,
    adt_v,
    mid_v,
    bo_v,
    bi_v,
    nb_v,
    dp_v,
    dp_in,
    km_v,
    sums_v,
    sums_in,
    kv_v,
    dg_v,
    ug_v,
    send_sem,
    recv_sem,
    local_sem,
):
    rows, width = kept.shape
    depth = wk.shape[0]
    tokens, heads = ck.shape
    rank = upk.shape[0]
    s = lax.axis_index("section")
    z = lax.axis_index("tensor")
    ahead = lax.rem(s + 1, sections)
    behind = lax.rem(s + sections - 1, sections)
    used = [0, 0]

    def load(src, dst):
        copy = pltpu.make_async_copy(src, dst, local_sem.at[used[1]])
        used[1] += 1
        copy.start()
        return copy

    sent = []

    def remote(src, dst, k, section, tensor):
        return pltpu.make_async_remote_copy(
            src_ref=src,
            dst_ref=dst,
            send_sem=send_sem.at[k],
            recv_sem=recv_sem.at[k],
            device_id=(section, tensor),
            device_id_type=MESH,
        )

    def send(src, dst, section, tensor):
        copy = remote(src, dst, used[0], section, tensor)
        used[0] += 1
        copy.start()
        sent.append(copy)
        return copy

    def head_cols(q):
        return pl.ds(pl.multiple_of(q * heads, heads), heads)

    def depth_cols(q):
        return pl.ds(pl.multiple_of(q * depth, depth), depth)

    bits = bits_up(count)
    own = [
        load(ck, cotk.at[:, head_cols(z)]),
        load(cv, cotv.at[:, head_cols(z)]),
        load(upk, upk_v.at[:, head_cols(z)]),
        load(upv, upv_v.at[:, head_cols(z)]),
    ]
    own_down = [load(dnk, dn_v.at[z, :rank]), load(dnv, dn_v.at[z, rank:])]
    arr_load = load(arr, arr_v)
    kept_load = load(kept, kept_v)
    weights = [load(wk, wk_v), load(wv, wv_v)]

    def inside(q):
        return (q >= 0) & (q < count)

    head_kinds = ((ck, cotk), (cv, cotv), (upk, upk_v), (upv, upv_v))
    guarded = []

    def relay(step, kinds):
        landing = []
        for way in (1, -1):
            q, to, come = z - way * (step - 1), z + way, z - way * step
            going = inside(q) & inside(to)
            for kind in kinds:
                if kind == 4:
                    src, dst, got = dn_v.at[q], dn_v.at[q], dn_v.at[come]
                else:
                    first, buf = head_kinds[kind]
                    dst, got = buf.at[:, head_cols(q)], buf.at[:, head_cols(come)]
                    src = first if step == 1 else dst
                k = used[0]
                used[0] += 1
                out = remote(src, dst, k, s, to)
                pl.when(going)(out.start)
                guarded.append((going, out))
                landing.append((kind, inside(come), remote(got, got, k, s, z)))
        return landing

    def landed(landing, kinds):
        for kind, coming, copy in landing:
            if kind in kinds:
                pl.when(coming)(copy.wait_recv)

    half = rows // halves
    ends = (z == 0) | (z == count - 1)

    def arriving(j, i):
        q = flip(z, j)
        at = pl.ds(i * half, half)
        copy = remote(arr.at[at, depth_cols(q)], x_v.at[z, at], used[0], ahead, q)
        used[0] += 1
        sent.append(copy)
        return copy

    far = list(range(max(bits[-1], 1), count)) if bits else []
    near = [j for j in range(1, count) if j not in far]
    arrivals = {(j, i): arriving(j, i) for j in range(count) for i in range(halves)}

    def start_near():
        for i in range(halves):
            for j in near:
                arrivals[j, i].start()

    def start_far(i):
        for j in far:
            arrivals[j, i].start()

    heads_only, down_only = (0, 1, 2, 3), (4,)
    landing = relay(1, heads_only) if bits else []
    for i in range(halves):
        arrivals[0, i].start()
    returned = send(ret, back_v, behind, z)
    for copy in own_down:
        copy.wait()
    landing += relay(1, down_only) if bits else []
    pl.when(ends)(start_near)

    arr_load.wait()

    def arr_stats(i, _):
        at = pl.ds(pl.multiple_of(i * row_tile, row_tile), row_tile)
        x = arr_v[at, :].astype(f32)
        inverse = lax.rsqrt(jnp.mean(x * x, axis=-1, keepdims=True) + epsilon)
        inv_t[at, :] = jnp.broadcast_to(inverse, (row_tile, lanes))
        return 0

    lax.fori_loop(0, rows // row_tile, arr_stats, 0)
    inv_in[z] = inv_t[...].T[:8]
    inverses = [send(inv_in.at[z], inv_in.at[z + count], ahead, flip(z, j)) for j in range(count)]
    kept_load.wait()

    def kept_stats(i, _):
        at = pl.ds(pl.multiple_of(i * row_tile, row_tile), row_tile)
        x = kept_v[at, :].astype(f32)
        inverse = lax.rsqrt(jnp.mean(x * x, axis=-1, keepdims=True) + epsilon)
        inv_b[at, :] = jnp.broadcast_to(inverse, (row_tile, lanes))
        return 0

    for step in range(1, count):
        landed(landing, heads_only)
        ahead_of = relay(step + 1, heads_only) if step + 1 < count else []
        landed(landing, down_only)
        ahead_of += relay(step + 1, down_only) if step + 1 < count else []
        landing = ahead_of
        if step <= halves:
            start_far(step - 1)
        if step == 1:
            lax.fori_loop(0, rows // row_tile, kept_stats, 0)
        if step == max(count - 2, 1):
            pl.when(jnp.logical_not(ends))(start_near)
    for i in range(max(count - 1, 0), halves):
        start_far(i)
    if count == 1:
        lax.fori_loop(0, rows // row_tile, kept_stats, 0)
    for copy in own + weights:
        copy.wait()

    for r, (cot, up) in enumerate(((cotk, upk_v), (cotv, upv_v))):
        ad_v[:, r * rank : (r + 1) * rank] = adapter_scale * dot_nt(cot[...], up[...])
        adt_v[r * rank : (r + 1) * rank, :] = adapter_scale * dot_nt(up[...], cot[...])

    tile = min(512, depth)

    def branch_tile(i, _):
        at = pl.ds(pl.multiple_of(i * tile, tile), tile)
        total = dot_nn(ad_v[...].astype(bf16), dn_v[z, :, at])
        total = total + dot_nt(cotk[...], wk_v[at, :])
        total = total + dot_nt(cotv[...], wv_v[at, :])
        bo_v[:, :, at] = total.astype(bf16).reshape(count, rows, tile)
        return 0

    lax.fori_loop(0, depth // tile, branch_tile, 0)
    part = rows // parts
    others = far + near
    branches = {}

    def send_branch(i):
        at = pl.ds(i * part, part)
        for j in others:
            q = flip(z, j)
            branches[j, i] = send(bo_v.at[q, at], bi_v.at[z, at], s, q)

    send_branch(0)

    def own_branch(i, _):
        at = pl.ds(pl.multiple_of(i * row_tile, row_tile), row_tile)
        bi_v[z, at, :] = bo_v[z, at, :]
        return 0

    lax.fori_loop(0, rows // row_tile, own_branch, 0)

    mine = adt_v[:, pl.ds(pl.multiple_of(z * rows, rows), rows)].astype(bf16)

    km_v[z] = jnp.zeros((2 * rank, rows), f32)

    def kept_block(j, _):
        inverse = inv_b[:, :1]

        def normalize(i, _):
            at = pl.ds(pl.multiple_of(i * tile, tile), tile)
            cols = pl.ds(pl.multiple_of(j * depth + i * tile, tile), tile)
            part = kept_v[:, cols].astype(f32) * inverse * gain_ref[:, cols].astype(f32)
            nb_v[:, at] = part.astype(bf16)
            return 0

        lax.fori_loop(0, depth // tile, normalize, 0)
        km_v[z] += dot_nt(dn_v[j], nb_v[...])
        dp_v[j] = dot_nn(mine, nb_v[...]).astype(bf16)
        return 0

    lax.fori_loop(0, count, kept_block, 0)
    mids = [send(km_v.at[z], km_v.at[z], s, flip(z, j)) for j in range(1, count)]

    def scatter_stage(buf, landing, bit):
        to = flip(z, bit)
        offset = sum(count // (2 * b) for b in bits if b < bit)
        return [
            send(buf.at[flip(z, bit ^ m)], landing.at[offset + k], s, to)
            for k, m in enumerate(range(0, count, 2 * bit))
        ]

    def scatter_add(buf, landing, bit, copies):
        offset = sum(count // (2 * b) for b in bits if b < bit)
        for k, m in enumerate(range(0, count, 2 * bit)):
            copies[k].wait_recv()
            q = flip(z, m)
            buf[q] = (buf[q].astype(f32) + landing[offset + k].astype(f32)).astype(bf16)

    stores = []
    down_stage = scatter_stage(dp_v, dp_in, bits[0]) if bits else []

    def head_block(q):
        gain_cols = depth_cols(z)

        def scale(i, _):
            at = pl.ds(pl.multiple_of(i * row_tile, row_tile), row_tile)
            x_v[q, at, :] = (x_v[q, at, :].astype(f32) * gain_ref[:, gain_cols].astype(f32)).astype(bf16)
            return 0

        lax.fori_loop(0, rows // row_tile, scale, 0)
        mid = adapter_scale * dot_nt(x_v[q], dn_v[z])
        mid_v[...] = mid.astype(bf16)
        at = pl.ds(pl.multiple_of(q * rows, rows), rows)

        def head_cut(d, _):
            cols = head_cols(d)
            for r, (w, up) in enumerate(((wk_v, upk_v), (wv_v, upv_v))):
                total = dot_nn(x_v[q], w[:, cols])
                total = total + dot_nn(mid_v[:, r * rank : (r + 1) * rank], up[:, cols])
                sums_v[d, r, at, :] = total.astype(bf16)
            return 0

        lax.fori_loop(0, count, head_cut, 0)

    for j in [0] + far + near:
        for i in range(halves):
            arrivals[j, i].wait_recv()
        head_block(flip(z, j))
    for k, bit in enumerate(bits):
        stage = scatter_stage(sums_v, sums_in, bit)
        if k == 0:
            for i in range(1, parts):
                send_branch(i)
        scatter_add(dp_v, dp_in, bit, down_stage)
        if k + 1 < len(bits):
            down_stage = scatter_stage(dp_v, dp_in, bits[k + 1])
        if k + 1 < len(bits):
            scatter_add(sums_v, sums_in, bit, stage)

    dg_v[...] = dp_v[z].astype(f32)
    stores.append(load(dg_v.at[:rank], dgk_out))
    stores.append(load(dg_v.at[rank:], dgv_out))
    for copy in mids:
        copy.wait_recv()
    for r, cot in enumerate((cotk, cotv)):
        total = jnp.zeros((rank, heads), f32)
        for q in range(count):
            mid = (adapter_scale * km_v[q, r * rank : (r + 1) * rank, :]).astype(bf16)
            total = total + dot_nn(mid, cot[q * rows : (q + 1) * rows, head_cols(z)])
        ug_v[r] = total
    stores.append(load(ug_v.at[0], ugk_out))
    stores.append(load(ug_v.at[1], ugv_out))
    for copy in inverses:
        copy.wait_recv()
    for q in range(count):
        spread = jnp.broadcast_to(inv_in[count + q, :1, :], (lanes, rows)).T
        inv_f[q * rows : (q + 1) * rows, :] = spread
    returned.wait_recv()

    def grad_tile(i, _):
        at = pl.ds(pl.multiple_of(i * row_tile, row_tile), row_tile)
        inverse = inv_b[at, :1]
        inner = jnp.zeros((row_tile, 1), f32)
        for j in range(count):
            cols = slice(j * depth, (j + 1) * depth)
            scaled = gain_ref[:, cols].astype(f32) * bi_v[j, at, :].astype(f32)
            inner = inner + jnp.sum(kept_v[at, cols].astype(f32) * scaled, axis=-1, keepdims=True)
        pull = inverse * inverse * inverse * (inner / width)
        for j in range(count):
            cols = slice(j * depth, (j + 1) * depth)
            scaled = gain_ref[:, cols].astype(f32) * bi_v[j, at, :].astype(f32)
            value = back_v[at, cols].astype(f32) + inverse * scaled - kept_v[at, cols].astype(f32) * pull
            arr_v[at, cols] = value.astype(bf16)
        return 0

    def finish(i):
        for j in others:
            branches[j, i].wait_recv()
        lax.fori_loop(i * part // row_tile, (i + 1) * part // row_tile, grad_tile, 0)
        at = pl.ds(i * part, part)
        stores.append(load(arr_v.at[at], grad_out.at[at]))

    for i in range(parts):
        finish(i)

    if bits:
        stage[0].wait_recv()

    def head_tile(i, _):
        at = pl.ds(pl.multiple_of(i * row_tile, row_tile), row_tile)
        for r in range(2):
            total = sums_v[z, r, at, :].astype(f32)
            if bits:
                total = total + sums_in[count - 2, r, at, :].astype(f32)
            kv_v[r, at, :] = (inv_f[at, :1] * total).astype(bf16)
        return 0

    lax.fori_loop(0, tokens // row_tile, head_tile, 0)
    stores.append(load(kv_v.at[0], keys_out))
    stores.append(load(kv_v.at[1], values_out))
    for copy in sent:
        copy.wait_send()
    for going, copy in guarded:
        pl.when(going)(copy.wait_send)
    for copy in stores:
        copy.wait()


def run_layer(count, sections, arr, kept, ret, gain, wk, wv, dnk, dnv, upk, upv, ck, cv):
    rows, width = kept.shape
    depth, wide = wk.shape
    tokens, heads = ck.shape
    rank = upk.shape[0]
    copies = 10 * (count - 1) + halves * count + count + 1
    copies += parts * (count - 1) + 3 * (count - 1)
    hbm = pl.BlockSpec(memory_space=pl.ANY)
    landing = max(count - 1, 1)
    return pl.pallas_call(
        functools.partial(layer_kernel, count, sections),
        in_specs=[pl.BlockSpec(memory_space=pltpu.VMEM)] + [hbm] * 11,
        out_specs=[hbm] * 7,
        out_shape=[
            jax.ShapeDtypeStruct((tokens, heads), bf16),
            jax.ShapeDtypeStruct((tokens, heads), bf16),
            jax.ShapeDtypeStruct((rows, width), bf16),
            jax.ShapeDtypeStruct((rank, depth), f32),
            jax.ShapeDtypeStruct((rank, depth), f32),
            jax.ShapeDtypeStruct((rank, heads), f32),
            jax.ShapeDtypeStruct((rank, heads), f32),
        ],
        scratch_shapes=[
            pltpu.VMEM((depth, wide), bf16),
            pltpu.VMEM((depth, wide), bf16),
            pltpu.VMEM((tokens, wide), bf16),
            pltpu.VMEM((tokens, wide), bf16),
            pltpu.VMEM((rank, wide), bf16),
            pltpu.VMEM((rank, wide), bf16),
            pltpu.VMEM((count, 2 * rank, depth), bf16),
            pltpu.VMEM((rows, width), bf16),
            pltpu.VMEM((rows, width), bf16),
            pltpu.VMEM((rows, width), bf16),
            pltpu.VMEM((count, rows, depth), bf16),
            pltpu.VMEM((rows, lanes), f32),
            pltpu.VMEM((2 * count, 8, rows), f32),
            pltpu.VMEM((tokens, lanes), f32),
            pltpu.VMEM((rows, lanes), f32),
            pltpu.VMEM((tokens, 2 * rank), f32),
            pltpu.VMEM((2 * rank, tokens), f32),
            pltpu.VMEM((rows, 2 * rank), bf16),
            pltpu.VMEM((count, rows, depth), bf16),
            pltpu.VMEM((count, rows, depth), bf16),
            pltpu.VMEM((rows, depth), bf16),
            pltpu.VMEM((count, 2 * rank, depth), bf16),
            pltpu.VMEM((landing, 2 * rank, depth), bf16),
            pltpu.VMEM((count, 2 * rank, rows), f32),
            pltpu.VMEM((count, 2, tokens, heads), bf16),
            pltpu.VMEM((landing, 2, tokens, heads), bf16),
            pltpu.VMEM((2, tokens, heads), bf16),
            pltpu.VMEM((2 * rank, depth), f32),
            pltpu.VMEM((2, rank, heads), f32),
            pltpu.SemaphoreType.DMA((copies,)),
            pltpu.SemaphoreType.DMA((copies,)),
            pltpu.SemaphoreType.DMA((10 + 6 + parts,)),
        ],
        compiler_params=pltpu.CompilerParams(
            has_side_effects=True, vmem_limit_bytes=67043328
        ),
        cost_estimate=pl.CostEstimate(
            flops=8 * tokens * depth * wide, bytes_accessed=4 * depth * wide, transcendentals=0
        ),
        name="layer",
    )(gain, arr, kept, ret, wk, wv, dnk, dnv, upk, upv, ck, cv)


def on_device(
    arriving,
    kept_input,
    returning,
    norm_gain,
    key_weight,
    value_weight,
    key_down,
    value_down,
    key_up,
    value_up,
    key_cot,
    value_cot,
):
    keys, values, input_grad, dgk, dgv, ugk, ugv = run_layer(
        lax.axis_size("tensor"),
        lax.axis_size("section"),
        arriving[0],
        kept_input[0],
        returning[0],
        norm_gain,
        key_weight[0],
        value_weight[0],
        key_down[0].T,
        value_down[0].T,
        key_up[0],
        value_up[0],
        key_cot[0],
        value_cot[0],
    )
    return (
        keys[None],
        values[None],
        input_grad[None],
        dgk.T[None],
        dgv.T[None],
        ugk[None],
        ugv[None],
    )


def solution(mesh):
    return jax.shard_map(
        on_device,
        mesh=mesh,
        in_specs=(
            P("section", "tensor", None),
            P("section", "tensor", None),
            P("section", "tensor", None),
            P("section", None),
            P("section", "tensor", None),
            P("section", "tensor", None),
            P("section", "tensor", None),
            P("section", "tensor", None),
            P("section", None, "tensor"),
            P("section", None, "tensor"),
            P("section", None, "tensor"),
            P("section", None, "tensor"),
        ),
        out_specs=(
            P("section", None, "tensor"),
            P("section", None, "tensor"),
            P("section", "tensor", None),
            P("section", "tensor", None),
            P("section", "tensor", None),
            P("section", None, "tensor"),
            P("section", None, "tensor"),
        ),
        check_vma=False,
    )
```

```python
import functools

import jax
import jax.numpy as jnp
from jax import lax
from jax.experimental import pallas as pl
from jax.experimental.pallas import tpu as pltpu
from jax.sharding import PartitionSpec as P

epsilon = 1e-05
adapter_scale = 2.0
bf16 = jnp.bfloat16
f32 = jnp.float32
MESH = pl.DeviceIdType.MESH
lanes = 128
parts = 4
halves = 2
row_tile = 16
kernel_mib = 55
store_mib = 16
store_tile = 128


def flip(z, mask):
    bit = 1
    while bit <= mask:
        if mask & bit:
            z = z + bit - 2 * bit * ((z // bit) % 2)
        bit *= 2
    return z


def bits_up(count):
    bits = []
    bit = 1
    while bit < count:
        bits.append(bit)
        bit *= 2
    return bits


def dot_nt(a, b):
    return lax.dot_general(a, b, (((1,), (1,)), ((), ())), preferred_element_type=f32)


def dot_nn(a, b):
    return jnp.dot(a, b, preferred_element_type=f32)


def layer_kernel(
    count,
    sections,
    gain,
    arr,
    kept,
    ret,
    wk,
    wv,
    dnk,
    dnv,
    upk,
    upv,
    ck,
    cv,
    own_out,
    sum_out,
    inv_f,
    grad_out,
    dgk_out,
    dgv_out,
    ugk_out,
    ugv_out,
    gain_ref,
    wk_v,
    wv_v,
    cotk,
    cotv,
    upk_v,
    upv_v,
    dn_v,
    arr_v,
    kept_v,
    back_v,
    x_v,
    inv_t,
    inv_in,
    inv_b,
    ad_v,
    adt_v,
    mid_v,
    bo_v,
    bi_v,
    nb_v,
    dp_v,
    dp_in,
    km_sum,
    km_v,
    sums_v,
    sums_in,
    send_sem,
    recv_sem,
    local_sem,
):
    rows, width = kept.shape
    depth = wk.shape[0]
    tokens, heads = ck.shape
    rank = upk.shape[0]
    s = lax.axis_index("section")
    z = lax.axis_index("tensor")
    ahead = lax.rem(s + 1, sections)
    behind = lax.rem(s + sections - 1, sections)
    used = [0, 0]

    def load(src, dst):
        copy = pltpu.make_async_copy(src, dst, local_sem.at[used[1]])
        used[1] += 1
        copy.start()
        return copy

    sent = []

    def remote(src, dst, k, section, tensor):
        return pltpu.make_async_remote_copy(
            src_ref=src,
            dst_ref=dst,
            send_sem=send_sem.at[k],
            recv_sem=recv_sem.at[k],
            device_id=(section, tensor),
            device_id_type=MESH,
        )

    def send(src, dst, section, tensor):
        copy = remote(src, dst, used[0], section, tensor)
        used[0] += 1
        copy.start()
        sent.append(copy)
        return copy

    def head_cols(q):
        return pl.ds(pl.multiple_of(q * heads, heads), heads)

    def depth_cols(q):
        return pl.ds(pl.multiple_of(q * depth, depth), depth)

    greet = [(s, flip(z, j)) for j in range(1, count)]
    greet += [(behind, flip(z, j)) for j in range(count)] + [(ahead, z)]
    entry = pltpu.get_barrier_semaphore()
    for peer in greet:
        pl.semaphore_signal(entry, inc=1, device_id=peer, device_id_type=MESH)
    pl.semaphore_wait(entry, len(greet))

    bits = bits_up(count)
    own = [
        load(ck, cotk.at[:, head_cols(z)]),
        load(cv, cotv.at[:, head_cols(z)]),
        load(upk, upk_v.at[:, head_cols(z)]),
        load(upv, upv_v.at[:, head_cols(z)]),
    ]
    own_down = [load(dnk, dn_v.at[z, :rank]), load(dnv, dn_v.at[z, rank:])]
    arr_load = load(arr, arr_v)
    kept_load = load(kept, kept_v)
    weights = [load(gain, gain_ref), load(wk, wk_v), load(wv, wv_v)]

    def inside(q):
        return (q >= 0) & (q < count)

    head_kinds = ((ck, cotk), (cv, cotv), (upk, upk_v), (upv, upv_v))
    guarded = []

    def relay(step, kinds):
        landing = []
        for way in (1, -1):
            q, to, come = z - way * (step - 1), z + way, z - way * step
            going = inside(q) & inside(to)
            for kind in kinds:
                if kind == 4:
                    src, dst, got = dn_v.at[q], dn_v.at[q], dn_v.at[come]
                else:
                    first, buf = head_kinds[kind]
                    dst, got = buf.at[:, head_cols(q)], buf.at[:, head_cols(come)]
                    src = first if step == 1 else dst
                k = used[0]
                used[0] += 1
                out = remote(src, dst, k, s, to)
                pl.when(going)(out.start)
                guarded.append((going, out))
                landing.append((kind, inside(come), remote(got, got, k, s, z)))
        return landing

    def landed(landing, kinds):
        for kind, coming, copy in landing:
            if kind in kinds:
                pl.when(coming)(copy.wait_recv)

    half = rows // halves
    ends = (z == 0) | (z == count - 1)

    def arriving(j, i):
        q = flip(z, j)
        at = pl.ds(i * half, half)
        copy = remote(arr.at[at, depth_cols(q)], x_v.at[z, at], used[0], ahead, q)
        used[0] += 1
        sent.append(copy)
        return copy

    far = list(range(max(bits[-1], 1), count)) if bits else []
    near = [j for j in range(1, count) if j not in far]
    arrivals = {(j, i): arriving(j, i) for j in range(count) for i in range(halves)}

    def start_near():
        for i in range(halves):
            for j in near:
                arrivals[j, i].start()

    def start_far(i):
        for j in far:
            arrivals[j, i].start()

    heads_only, down_only = (0, 1, 2, 3), (4,)
    landing = relay(1, heads_only) if bits else []
    for i in range(halves):
        arrivals[0, i].start()
    returned = send(ret, back_v, behind, z)
    for copy in own_down:
        copy.wait()
    landing += relay(1, down_only) if bits else []
    pl.when(ends)(start_near)

    arr_load.wait()

    def arr_stats(i, _):
        at = pl.ds(pl.multiple_of(i * row_tile, row_tile), row_tile)
        x = arr_v[at, :].astype(f32)
        inverse = lax.rsqrt(jnp.mean(x * x, axis=-1, keepdims=True) + epsilon)
        inv_t[at, :] = jnp.broadcast_to(inverse, (row_tile, lanes))
        return 0

    lax.fori_loop(0, rows // row_tile, arr_stats, 0)
    inv_in[z] = inv_t[...].T[:8]
    inverses = [send(inv_in.at[z], inv_in.at[z + count], ahead, flip(z, j)) for j in range(count)]
    kept_load.wait()

    def kept_stats(i, _):
        at = pl.ds(pl.multiple_of(i * row_tile, row_tile), row_tile)
        x = kept_v[at, :].astype(f32)
        inverse = lax.rsqrt(jnp.mean(x * x, axis=-1, keepdims=True) + epsilon)
        inv_b[at, :] = jnp.broadcast_to(inverse, (row_tile, lanes))
        return 0

    for step in range(1, count):
        landed(landing, heads_only)
        ahead_of = relay(step + 1, heads_only) if step + 1 < count else []
        landed(landing, down_only)
        ahead_of += relay(step + 1, down_only) if step + 1 < count else []
        landing = ahead_of
        if step <= halves:
            start_far(step - 1)
        if step == 1:
            lax.fori_loop(0, rows // row_tile, kept_stats, 0)
        if step == max(count - 2, 1):
            pl.when(jnp.logical_not(ends))(start_near)
    for i in range(max(count - 1, 0), halves):
        start_far(i)
    if count == 1:
        lax.fori_loop(0, rows // row_tile, kept_stats, 0)
    for copy in own + weights:
        copy.wait()

    for r, (cot, up) in enumerate(((cotk, upk_v), (cotv, upv_v))):
        ad_v[:, r * rank : (r + 1) * rank] = adapter_scale * dot_nt(cot[...], up[...])
        adt_v[r * rank : (r + 1) * rank, :] = adapter_scale * dot_nt(up[...], cot[...])

    tile = min(512, depth)

    def branch_tile(i, _):
        at = pl.ds(pl.multiple_of(i * tile, tile), tile)
        total = dot_nn(ad_v[...].astype(bf16), dn_v[z, :, at])
        total = total + dot_nt(cotk[...], wk_v[at, :])
        total = total + dot_nt(cotv[...], wv_v[at, :])
        bo_v[:, :, at] = total.astype(bf16).reshape(count, rows, tile)
        return 0

    lax.fori_loop(0, depth // tile, branch_tile, 0)
    part = rows // parts
    others = far + near
    branches = {}

    def send_branch(i):
        at = pl.ds(i * part, part)
        for j in others:
            q = flip(z, j)
            branches[j, i] = send(bo_v.at[q, at], bi_v.at[z, at], s, q)

    send_branch(0)

    def own_branch(i, _):
        at = pl.ds(pl.multiple_of(i * row_tile, row_tile), row_tile)
        bi_v[z, at, :] = bo_v[z, at, :]
        return 0

    lax.fori_loop(0, rows // row_tile, own_branch, 0)

    mine = adt_v[:, pl.ds(pl.multiple_of(z * rows, rows), rows)].astype(bf16)

    km_sum[...] = jnp.zeros((2 * rank, rows), f32)

    def kept_block(j, _):
        inverse = inv_b[:, :1]

        def normalize(i, _):
            at = pl.ds(pl.multiple_of(i * tile, tile), tile)
            cols = pl.ds(pl.multiple_of(j * depth + i * tile, tile), tile)
            part = kept_v[:, cols].astype(f32) * inverse * gain_ref[:, cols].astype(f32)
            nb_v[:, at] = part.astype(bf16)
            return 0

        lax.fori_loop(0, depth // tile, normalize, 0)
        km_sum[...] += dot_nt(dn_v[j], nb_v[...])
        dp_v[j] = dot_nn(mine, nb_v[...]).astype(bf16)
        return 0

    lax.fori_loop(0, count, kept_block, 0)
    km_v[z] = (adapter_scale * km_sum[...]).astype(bf16)
    mids = [send(km_v.at[z], km_v.at[z], s, flip(z, j)) for j in range(1, count)]

    def down_slot(k):
        return dp_in.at[k]

    def sum_slot(k):
        return sum_out if k == count - 2 else sums_in.at[k]

    def scatter_stage(buf, landing, bit):
        to = flip(z, bit)
        offset = sum(count // (2 * b) for b in bits if b < bit)
        return [
            send(buf.at[flip(z, bit ^ m)], landing(offset + k), s, to)
            for k, m in enumerate(range(0, count, 2 * bit))
        ]

    def scatter_add(buf, landing, bit, copies):
        offset = sum(count // (2 * b) for b in bits if b < bit)
        for k, m in enumerate(range(0, count, 2 * bit)):
            copies[k].wait_recv()
            q = flip(z, m)
            buf[q] = (buf[q].astype(f32) + landing(offset + k)[...].astype(f32)).astype(bf16)

    down_stage = scatter_stage(dp_v, down_slot, bits[0]) if bits else []

    def head_block(q):
        gain_cols = depth_cols(z)

        def scale(i, _):
            at = pl.ds(pl.multiple_of(i * row_tile, row_tile), row_tile)
            x_v[q, at, :] = (x_v[q, at, :].astype(f32) * gain_ref[:, gain_cols].astype(f32)).astype(bf16)
            return 0

        lax.fori_loop(0, rows // row_tile, scale, 0)
        mid = adapter_scale * dot_nt(x_v[q], dn_v[z])
        mid_v[...] = mid.astype(bf16)
        at = pl.ds(pl.multiple_of(q * rows, rows), rows)

        def head_cut(d, _):
            cols = head_cols(d)
            for r, (w, up) in enumerate(((wk_v, upk_v), (wv_v, upv_v))):
                total = dot_nn(x_v[q], w[:, cols])
                total = total + dot_nn(mid_v[:, r * rank : (r + 1) * rank], up[:, cols])
                sums_v[d, r, at, :] = total.astype(bf16)
            return 0

        lax.fori_loop(0, count, head_cut, 0)

    for j in [0] + far + near:
        for i in range(halves):
            arrivals[j, i].wait_recv()
        head_block(flip(z, j))
    for k, bit in enumerate(bits):
        stage = scatter_stage(sums_v, sum_slot, bit)
        if k == 0:
            for i in range(1, parts):
                send_branch(i)
        scatter_add(dp_v, down_slot, bit, down_stage)
        if k + 1 < len(bits):
            down_stage = scatter_stage(dp_v, down_slot, bits[k + 1])
        if k + 1 < len(bits):
            scatter_add(sums_v, sum_slot, bit, stage)

    dgk_out[...] = dp_v[z, :rank].astype(f32)
    dgv_out[...] = dp_v[z, rank:].astype(f32)
    for copy in mids:
        copy.wait_recv()
    for r, cot in enumerate((cotk, cotv)):
        total = jnp.zeros((rank, heads), f32)
        for q in range(count):
            mid = km_v[q, r * rank : (r + 1) * rank, :]
            total = total + dot_nn(mid, cot[q * rows : (q + 1) * rows, head_cols(z)])
        (ugk_out, ugv_out)[r][...] = total
    for copy in inverses:
        copy.wait_recv()
    for q in range(count):
        spread = jnp.broadcast_to(inv_in[count + q, :1, :], (lanes, rows)).T
        inv_f[q * rows : (q + 1) * rows, :] = spread
    own_out[...] = sums_v[z]
    returned.wait_recv()

    def grad_tile(i, _):
        at = pl.ds(pl.multiple_of(i * row_tile, row_tile), row_tile)
        inverse = inv_b[at, :1]
        inner = jnp.zeros((row_tile, 1), f32)
        for j in range(count):
            cols = slice(j * depth, (j + 1) * depth)
            scaled = gain_ref[:, cols].astype(f32) * bi_v[j, at, :].astype(f32)
            inner = inner + jnp.sum(kept_v[at, cols].astype(f32) * scaled, axis=-1, keepdims=True)
        pull = inverse * inverse * inverse * (inner / width)
        for j in range(count):
            cols = slice(j * depth, (j + 1) * depth)
            scaled = gain_ref[:, cols].astype(f32) * bi_v[j, at, :].astype(f32)
            value = back_v[at, cols].astype(f32) + inverse * scaled - kept_v[at, cols].astype(f32) * pull
            grad_out[at, cols] = value.astype(bf16)
        return 0

    def finish(i):
        for j in others:
            branches[j, i].wait_recv()
        lax.fori_loop(i * part // row_tile, (i + 1) * part // row_tile, grad_tile, 0)

    for i in range(parts):
        finish(i)

    if bits:
        stage[0].wait_recv()
    else:
        sum_out[...] = jnp.zeros(sum_out.shape, bf16)
    for copy in sent:
        copy.wait_send()
    for going, copy in guarded:
        pl.when(going)(copy.wait_send)


def run_layer(count, sections, arr, kept, ret, gain, wk, wv, dnk, dnv, upk, upv, ck, cv):
    rows, width = kept.shape
    depth, wide = wk.shape
    tokens, heads = ck.shape
    rank = upk.shape[0]
    copies = 10 * (count - 1) + halves * count + count + 1
    copies += parts * (count - 1) + 3 * (count - 1)
    hbm = pl.BlockSpec(memory_space=pl.ANY)
    landing = max(count - 1, 1)
    return pl.pallas_call(
        functools.partial(layer_kernel, count, sections),
        in_specs=[hbm] * 12,
        out_specs=[pl.BlockSpec(memory_space=pltpu.VMEM)] * 8,
        out_shape=[
            pltpu.VMEM((2, tokens, heads), bf16),
            pltpu.VMEM((2, tokens, heads), bf16),
            pltpu.VMEM((tokens, lanes), f32),
            pltpu.VMEM((rows, width), bf16),
            pltpu.VMEM((rank, depth), f32),
            pltpu.VMEM((rank, depth), f32),
            pltpu.VMEM((rank, heads), f32),
            pltpu.VMEM((rank, heads), f32),
        ],
        scratch_shapes=[
            pltpu.VMEM((1, width), bf16),
            pltpu.VMEM((depth, wide), bf16),
            pltpu.VMEM((depth, wide), bf16),
            pltpu.VMEM((tokens, wide), bf16),
            pltpu.VMEM((tokens, wide), bf16),
            pltpu.VMEM((rank, wide), bf16),
            pltpu.VMEM((rank, wide), bf16),
            pltpu.VMEM((count, 2 * rank, depth), bf16),
            pltpu.VMEM((rows, width), bf16),
            pltpu.VMEM((rows, width), bf16),
            pltpu.VMEM((rows, width), bf16),
            pltpu.VMEM((count, rows, depth), bf16),
            pltpu.VMEM((rows, lanes), f32),
            pltpu.VMEM((2 * count, 8, rows), f32),
            pltpu.VMEM((rows, lanes), f32),
            pltpu.VMEM((tokens, 2 * rank), f32),
            pltpu.VMEM((2 * rank, tokens), f32),
            pltpu.VMEM((rows, 2 * rank), bf16),
            pltpu.VMEM((count, rows, depth), bf16),
            pltpu.VMEM((count, rows, depth), bf16),
            pltpu.VMEM((rows, depth), bf16),
            pltpu.VMEM((count, 2 * rank, depth), bf16),
            pltpu.VMEM((landing, 2 * rank, depth), bf16),
            pltpu.VMEM((2 * rank, rows), f32),
            pltpu.VMEM((count, 2 * rank, rows), bf16),
            pltpu.VMEM((count, 2, tokens, heads), bf16),
            pltpu.VMEM((max(count - 2, 1), 2, tokens, heads), bf16),
            pltpu.SemaphoreType.DMA((copies,)),
            pltpu.SemaphoreType.DMA((copies,)),
            pltpu.SemaphoreType.DMA((11,)),
        ],
        compiler_params=pltpu.CompilerParams(
            has_side_effects=True, collective_id=0, vmem_limit_bytes=kernel_mib * 2**20
        ),
        cost_estimate=pl.CostEstimate(
            flops=8 * tokens * depth * wide, bytes_accessed=4 * depth * wide, transcendentals=0
        ),
        name="layer",
    )(gain, arr, kept, ret, wk, wv, dnk, dnv, upk, upv, ck, cv)


def store_kernel(cuts, own, got, inv, grad, dgk, dgv, ugk, ugv, *refs):
    outs, (keys_v, values_v, sem) = refs[:7], refs[7:]
    copies = []

    def store(src, dst):
        copies.append(pltpu.make_async_copy(src, dst, sem.at[len(copies)]))
        copies[-1].start()

    step = grad.shape[0] // cuts
    for i in range(cuts):
        at = pl.ds(i * step, step)
        store(grad.at[at], outs[2].at[at])
    for src, dst in zip((dgk, dgv, ugk, ugv), outs[3:]):
        store(src, dst)
    for r, head in enumerate((keys_v, values_v)):

        cut = min(store_tile, head.shape[0])
        for i in range(0, head.shape[0], cut):
            at = slice(i, i + cut)
            total = own[r, at, :].astype(f32) + got[r, at, :].astype(f32)
            head[at, :] = (inv[at, :1] * total).astype(bf16)
        store(head, outs[r])
    for copy in copies:
        copy.wait()


def store(results):
    own, _, _, *rest = results
    head = jax.ShapeDtypeStruct(own.shape[1:], bf16)
    cuts = 4
    return pl.pallas_call(
        functools.partial(store_kernel, cuts),
        in_specs=[pl.BlockSpec(memory_space=pltpu.VMEM)] * len(results),
        out_specs=[pl.BlockSpec(memory_space=pl.ANY)] * 7,
        out_shape=[head, head] + [jax.ShapeDtypeStruct(x.shape, x.dtype) for x in rest],
        scratch_shapes=[pltpu.VMEM(head.shape, bf16)] * 2
        + [pltpu.SemaphoreType.DMA((cuts + 6,))],
        compiler_params=pltpu.CompilerParams(vmem_limit_bytes=store_mib * 2**20),
        name="store",
    )(*results)


def on_device(
    arriving,
    kept_input,
    returning,
    norm_gain,
    key_weight,
    value_weight,
    key_down,
    value_down,
    key_up,
    value_up,
    key_cot,
    value_cot,
):
    keys, values, input_grad, dgk, dgv, ugk, ugv = store(run_layer(
        lax.axis_size("tensor"),
        lax.axis_size("section"),
        arriving[0],
        kept_input[0],
        returning[0],
        norm_gain,
        key_weight[0],
        value_weight[0],
        key_down[0].T,
        value_down[0].T,
        key_up[0],
        value_up[0],
        key_cot[0],
        value_cot[0],
    ))
    return (
        keys[None],
        values[None],
        input_grad[None],
        dgk.T[None],
        dgv.T[None],
        ugk[None],
        ugv[None],
    )


def solution(mesh):
    return jax.shard_map(
        on_device,
        mesh=mesh,
        in_specs=(
            P("section", "tensor", None),
            P("section", "tensor", None),
            P("section", "tensor", None),
            P("section", None),
            P("section", "tensor", None),
            P("section", "tensor", None),
            P("section", "tensor", None),
            P("section", "tensor", None),
            P("section", None, "tensor"),
            P("section", None, "tensor"),
            P("section", None, "tensor"),
            P("section", None, "tensor"),
        ),
        out_specs=(
            P("section", None, "tensor"),
            P("section", None, "tensor"),
            P("section", "tensor", None),
            P("section", "tensor", None),
            P("section", "tensor", None),
            P("section", None, "tensor"),
            P("section", None, "tensor"),
        ),
        check_vma=False,
    )
```

```python
import functools

import jax
import jax.numpy as jnp
from jax import lax
from jax.experimental import pallas as pl
from jax.experimental.pallas import tpu as pltpu
from jax.sharding import PartitionSpec as P

epsilon = 1e-05
adapter_scale = 2.0
bf16 = jnp.bfloat16
f32 = jnp.float32
MESH = pl.DeviceIdType.MESH
lanes = 128
cuts_of_16 = (0, 4, 8, 12, 14, 16)
parts = len(cuts_of_16) - 1
halves = 2
row_tile = 16
kernel_mib = 55
store_mib = 16
store_tile = 128


def flip(z, mask):
    bit = 1
    while bit <= mask:
        if mask & bit:
            z = z + bit - 2 * bit * ((z // bit) % 2)
        bit *= 2
    return z


def bits_up(count):
    bits = []
    bit = 1
    while bit < count:
        bits.append(bit)
        bit *= 2
    return bits


def dot_nt(a, b):
    return lax.dot_general(a, b, (((1,), (1,)), ((), ())), preferred_element_type=f32)


def dot_nn(a, b):
    return jnp.dot(a, b, preferred_element_type=f32)


def layer_kernel(
    count,
    sections,
    gain,
    arr,
    kept,
    ret,
    wk,
    wv,
    dnk,
    dnv,
    upk,
    upv,
    ck,
    cv,
    own_out,
    sum_out,
    inv_f,
    grad_out,
    dgk_out,
    dgv_out,
    ugk_out,
    ugv_out,
    gain_ref,
    wk_v,
    wv_v,
    cotk,
    cotv,
    upk_v,
    upv_v,
    dn_v,
    arr_v,
    kept_v,
    back_v,
    x_v,
    inv_t,
    inv_in,
    inv_b,
    ad_v,
    adt_v,
    mid_v,
    bo_v,
    bi_v,
    nb_v,
    dp_v,
    dp_in,
    km_sum,
    km_v,
    sums_v,
    sums_in,
    send_sem,
    recv_sem,
    local_sem,
):
    rows, width = kept.shape
    depth = wk.shape[0]
    tokens, heads = ck.shape
    rank = upk.shape[0]
    s = lax.axis_index("section")
    z = lax.axis_index("tensor")
    ahead = lax.rem(s + 1, sections)
    behind = lax.rem(s + sections - 1, sections)
    used = [0, 0]

    def load(src, dst):
        copy = pltpu.make_async_copy(src, dst, local_sem.at[used[1]])
        used[1] += 1
        copy.start()
        return copy

    sent = []

    def remote(src, dst, k, section, tensor):
        return pltpu.make_async_remote_copy(
            src_ref=src,
            dst_ref=dst,
            send_sem=send_sem.at[k],
            recv_sem=recv_sem.at[k],
            device_id=(section, tensor),
            device_id_type=MESH,
        )

    def later(src, dst, section, tensor):
        copy = remote(src, dst, used[0], section, tensor)
        used[0] += 1
        sent.append(copy)
        return copy

    def send(src, dst, section, tensor):
        copy = later(src, dst, section, tensor)
        copy.start()
        return copy

    def head_cols(q):
        return pl.ds(pl.multiple_of(q * heads, heads), heads)

    def depth_cols(q):
        return pl.ds(pl.multiple_of(q * depth, depth), depth)

    greet = [(s, flip(z, j)) for j in range(1, count)]
    greet += [(behind, flip(z, j)) for j in range(count)] + [(ahead, z)]
    entry = pltpu.get_barrier_semaphore()
    for peer in greet:
        pl.semaphore_signal(entry, inc=1, device_id=peer, device_id_type=MESH)

    bits = bits_up(count)
    own = [
        load(ck, cotk.at[:, head_cols(z)]),
        load(cv, cotv.at[:, head_cols(z)]),
        load(upk, upk_v.at[:, head_cols(z)]),
        load(upv, upv_v.at[:, head_cols(z)]),
    ]
    own_down = [load(dnk, dn_v.at[z, :rank]), load(dnv, dn_v.at[z, rank:])]
    arr_load = load(arr, arr_v)
    kept_load = load(kept, kept_v)
    weights = [load(gain, gain_ref), load(wk, wk_v), load(wv, wv_v)]
    for copy in own + own_down:
        copy.wait()
    pl.semaphore_wait(entry, len(greet))

    def inside(q):
        return (q >= 0) & (q < count)

    head_kinds = (cotk, cotv, upk_v, upv_v)
    guarded = []

    def relay(step, kinds):
        landing = []
        for way in (1, -1):
            q, to, come = z - way * (step - 1), z + way, z - way * step
            going = inside(q) & inside(to)
            for kind in kinds:
                if kind == 4:
                    block, got = dn_v.at[q], dn_v.at[come]
                else:
                    buf = head_kinds[kind]
                    block, got = buf.at[:, head_cols(q)], buf.at[:, head_cols(come)]
                k = used[0]
                used[0] += 1
                out = remote(block, block, k, s, to)
                pl.when(going)(out.start)
                guarded.append((going, out))
                landing.append((kind, inside(come), remote(got, got, k, s, z)))
        return landing

    def landed(landing, kinds):
        for kind, coming, copy in landing:
            if kind in kinds:
                pl.when(coming)(copy.wait_recv)

    half = rows // halves
    ends = (z == 0) | (z == count - 1)

    def arriving(j, i):
        q = flip(z, j)
        at = pl.ds(i * half, half)
        return later(arr.at[at, depth_cols(q)], x_v.at[z, at], ahead, q)

    far = list(range(max(bits[-1], 1), count)) if bits else []
    near = [j for j in range(1, count) if j not in far]
    arrivals = {(j, i): arriving(j, i) for j in range(count) for i in range(halves)}

    def start_near():
        for i in range(halves):
            for j in near:
                arrivals[j, i].start()

    def start_far(i):
        for j in far:
            arrivals[j, i].start()

    heads_only, down_only = (0, 1, 2, 3), (4,)
    landing = relay(1, heads_only) if bits else []
    for i in range(halves):
        arrivals[0, i].start()
    returned = send(ret, back_v, behind, z)
    landing += relay(1, down_only) if bits else []
    pl.when(ends)(start_near)

    arr_load.wait()

    def arr_stats(i, _):
        at = pl.ds(pl.multiple_of(i * row_tile, row_tile), row_tile)
        x = arr_v[at, :].astype(f32)
        inverse = lax.rsqrt(jnp.mean(x * x, axis=-1, keepdims=True) + epsilon)
        inv_t[at, :] = jnp.broadcast_to(inverse, (row_tile, lanes))
        return 0

    lax.fori_loop(0, rows // row_tile, arr_stats, 0)
    inv_in[z] = inv_t[...].T[:8]
    inverses = [send(inv_in.at[z], inv_in.at[z + count], ahead, flip(z, j)) for j in range(count)]
    kept_load.wait()

    def kept_stats(i, _):
        at = pl.ds(pl.multiple_of(i * row_tile, row_tile), row_tile)
        x = kept_v[at, :].astype(f32)
        inverse = lax.rsqrt(jnp.mean(x * x, axis=-1, keepdims=True) + epsilon)
        inv_b[at, :] = jnp.broadcast_to(inverse, (row_tile, lanes))
        return 0

    for step in range(1, count):
        landed(landing, heads_only)
        ahead_of = relay(step + 1, heads_only) if step + 1 < count else []
        landed(landing, down_only)
        ahead_of += relay(step + 1, down_only) if step + 1 < count else []
        landing = ahead_of
        if step <= halves:
            start_far(step - 1)
        if step == 1:
            lax.fori_loop(0, rows // row_tile, kept_stats, 0)
        if step == max(count - 2, 1):
            pl.when(jnp.logical_not(ends))(start_near)
    for i in range(max(count - 1, 0), halves):
        start_far(i)
    if count == 1:
        lax.fori_loop(0, rows // row_tile, kept_stats, 0)
    for copy in weights:
        copy.wait()

    for r, (cot, up) in enumerate(((cotk, upk_v), (cotv, upv_v))):
        ad_v[:, r * rank : (r + 1) * rank] = adapter_scale * dot_nt(cot[...], up[...])
        adt_v[r * rank : (r + 1) * rank, :] = adapter_scale * dot_nt(up[...], cot[...])

    tile = min(512, depth)

    def branch_tile(i, _):
        at = pl.ds(pl.multiple_of(i * tile, tile), tile)
        total = dot_nn(ad_v[...].astype(bf16), dn_v[z, :, at])
        total = total + dot_nt(cotk[...], wk_v[at, :])
        total = total + dot_nt(cotv[...], wv_v[at, :])
        bo_v[:, :, at] = total.astype(bf16).reshape(count, rows, tile)
        return 0

    lax.fori_loop(0, depth // tile, branch_tile, 0)
    cuts = [rows * cut // 16 for cut in cuts_of_16]
    others = far + near

    def branch(j, i):
        at = pl.ds(cuts[i], cuts[i + 1] - cuts[i])
        q = flip(z, j)
        return later(bo_v.at[q, at], bi_v.at[z, at], s, q)

    branches = {(j, i): branch(j, i) for j in others for i in range(parts)}

    held_back = (count - 1, parts - 1)

    def send_branches(group):
        for i in range(1, parts):
            for j in group:
                if group is others or (j, i) != held_back:
                    branches[j, i].start()

    for j in others:
        branches[j, 0].start()
    pl.when(jnp.logical_not(ends))(functools.partial(send_branches, far))

    def own_branch(i, _):
        at = pl.ds(pl.multiple_of(i * row_tile, row_tile), row_tile)
        bi_v[z, at, :] = bo_v[z, at, :]
        return 0

    lax.fori_loop(0, rows // row_tile, own_branch, 0)

    mine = adt_v[:, pl.ds(pl.multiple_of(z * rows, rows), rows)].astype(bf16)

    km_sum[...] = jnp.zeros((2 * rank, rows), f32)

    def kept_block(j, _):
        inverse = inv_b[:, :1]

        def normalize(i, _):
            at = pl.ds(pl.multiple_of(i * tile, tile), tile)
            cols = pl.ds(pl.multiple_of(j * depth + i * tile, tile), tile)
            part = kept_v[:, cols].astype(f32) * inverse * gain_ref[:, cols].astype(f32)
            nb_v[:, at] = part.astype(bf16)
            return 0

        lax.fori_loop(0, depth // tile, normalize, 0)
        km_sum[...] += dot_nt(dn_v[j], nb_v[...])
        dp_v[j] = dot_nn(mine, nb_v[...]).astype(bf16)
        return 0

    lax.fori_loop(0, count, kept_block, 0)
    km_v[z] = (adapter_scale * km_sum[...]).astype(bf16)
    mids = [send(km_v.at[z], km_v.at[z], s, flip(z, j)) for j in range(1, count)]

    def down_slot(k):
        return dp_in.at[k]

    def sum_slot(k):
        return sum_out if k == count - 2 else sums_in.at[k]

    def scatter_stage(buf, landing, bit):
        to = flip(z, bit)
        offset = sum(count // (2 * b) for b in bits if b < bit)
        return [
            send(buf.at[flip(z, bit ^ m)], landing(offset + k), s, to)
            for k, m in enumerate(range(0, count, 2 * bit))
        ]

    def scatter_add(buf, landing, bit, copies):
        offset = sum(count // (2 * b) for b in bits if b < bit)
        for k, m in enumerate(range(0, count, 2 * bit)):
            copies[k].wait_recv()
            q = flip(z, m)
            buf[q] = (buf[q].astype(f32) + landing(offset + k)[...].astype(f32)).astype(bf16)

    down_stage = scatter_stage(dp_v, down_slot, bits[0]) if bits else []

    def head_block(q):
        gain_cols = depth_cols(z)

        def scale(i, _):
            at = pl.ds(pl.multiple_of(i * row_tile, row_tile), row_tile)
            x_v[q, at, :] = (x_v[q, at, :].astype(f32) * gain_ref[:, gain_cols].astype(f32)).astype(bf16)
            return 0

        lax.fori_loop(0, rows // row_tile, scale, 0)
        mid = adapter_scale * dot_nt(x_v[q], dn_v[z])
        mid_v[...] = mid.astype(bf16)
        at = pl.ds(pl.multiple_of(q * rows, rows), rows)

        def head_cut(d, _):
            cols = head_cols(d)
            for r, (w, up) in enumerate(((wk_v, upk_v), (wv_v, upv_v))):
                total = dot_nn(x_v[q], w[:, cols])
                total = total + dot_nn(mid_v[:, r * rank : (r + 1) * rank], up[:, cols])
                sums_v[d, r, at, :] = total.astype(bf16)
            return 0

        lax.fori_loop(0, count, head_cut, 0)

    for j in [0] + far + near:
        for i in range(halves):
            arrivals[j, i].wait_recv()
        head_block(flip(z, j))
    for k, bit in enumerate(bits):
        stage = scatter_stage(sums_v, sum_slot, bit)
        if k == 0:
            pl.when(ends)(functools.partial(send_branches, others))
            pl.when(jnp.logical_not(ends))(functools.partial(send_branches, near))
        if k + 1 < len(bits):
            scatter_add(dp_v, down_slot, bit, down_stage)
            down_stage = scatter_stage(dp_v, down_slot, bits[k + 1])
            scatter_add(sums_v, sum_slot, bit, stage)

    if others:
        pl.when(jnp.logical_not(ends))(branches[held_back].start)
    for copy in mids:
        copy.wait_recv()
    for r, cot in enumerate((cotk, cotv)):
        total = jnp.zeros((rank, heads), f32)
        for q in range(count):
            mid = km_v[q, r * rank : (r + 1) * rank, :]
            total = total + dot_nn(mid, cot[q * rows : (q + 1) * rows, head_cols(z)])
        (ugk_out, ugv_out)[r][...] = total
    for copy in inverses:
        copy.wait_recv()
    for q in range(count):
        spread = jnp.broadcast_to(inv_in[count + q, :1, :], (lanes, rows)).T
        inv_f[q * rows : (q + 1) * rows, :] = spread
    own_out[...] = sums_v[z]
    returned.wait_recv()

    def grad_tile(i, _):
        at = pl.ds(pl.multiple_of(i * row_tile, row_tile), row_tile)
        inverse = inv_b[at, :1]
        inner = jnp.zeros((row_tile, 1), f32)
        for j in range(count):
            cols = slice(j * depth, (j + 1) * depth)
            scaled = gain_ref[:, cols].astype(f32) * bi_v[j, at, :].astype(f32)
            inner = inner + jnp.sum(kept_v[at, cols].astype(f32) * scaled, axis=-1, keepdims=True)
        pull = inverse * inverse * inverse * (inner / width)
        for j in range(count):
            cols = slice(j * depth, (j + 1) * depth)
            scaled = gain_ref[:, cols].astype(f32) * bi_v[j, at, :].astype(f32)
            value = back_v[at, cols].astype(f32) + inverse * scaled - kept_v[at, cols].astype(f32) * pull
            grad_out[at, cols] = value.astype(bf16)
        return 0

    def finish(i):
        for j in others:
            branches[j, i].wait_recv()
        lax.fori_loop(cuts[i] // row_tile, cuts[i + 1] // row_tile, grad_tile, 0)

    for i in range(parts - 1):
        finish(i)
    if bits:
        scatter_add(dp_v, down_slot, bits[-1], down_stage)
    dgk_out[...] = dp_v[z, :rank].astype(f32)
    dgv_out[...] = dp_v[z, rank:].astype(f32)
    finish(parts - 1)
    if bits:
        stage[0].wait_recv()
    else:
        sum_out[...] = jnp.zeros(sum_out.shape, bf16)
    for copy in sent:
        copy.wait_send()
    for going, copy in guarded:
        pl.when(going)(copy.wait_send)


def run_layer(count, sections, arr, kept, ret, gain, wk, wv, dnk, dnv, upk, upv, ck, cv):
    rows, width = kept.shape
    depth, wide = wk.shape
    tokens, heads = ck.shape
    rank = upk.shape[0]
    copies = 10 * (count - 1) + halves * count + count + 1
    copies += parts * (count - 1) + 3 * (count - 1)
    hbm = pl.BlockSpec(memory_space=pl.ANY)
    landing = max(count - 1, 1)
    return pl.pallas_call(
        functools.partial(layer_kernel, count, sections),
        in_specs=[hbm] * 12,
        out_specs=[pl.BlockSpec(memory_space=pltpu.VMEM)] * 8,
        out_shape=[
            pltpu.VMEM((2, tokens, heads), bf16),
            pltpu.VMEM((2, tokens, heads), bf16),
            pltpu.VMEM((tokens, lanes), f32),
            pltpu.VMEM((rows, width), bf16),
            pltpu.VMEM((rank, depth), f32),
            pltpu.VMEM((rank, depth), f32),
            pltpu.VMEM((rank, heads), f32),
            pltpu.VMEM((rank, heads), f32),
        ],
        scratch_shapes=[
            pltpu.VMEM((1, width), bf16),
            pltpu.VMEM((depth, wide), bf16),
            pltpu.VMEM((depth, wide), bf16),
            pltpu.VMEM((tokens, wide), bf16),
            pltpu.VMEM((tokens, wide), bf16),
            pltpu.VMEM((rank, wide), bf16),
            pltpu.VMEM((rank, wide), bf16),
            pltpu.VMEM((count, 2 * rank, depth), bf16),
            pltpu.VMEM((rows, width), bf16),
            pltpu.VMEM((rows, width), bf16),
            pltpu.VMEM((rows, width), bf16),
            pltpu.VMEM((count, rows, depth), bf16),
            pltpu.VMEM((rows, lanes), f32),
            pltpu.VMEM((2 * count, 8, rows), f32),
            pltpu.VMEM((rows, lanes), f32),
            pltpu.VMEM((tokens, 2 * rank), f32),
            pltpu.VMEM((2 * rank, tokens), f32),
            pltpu.VMEM((rows, 2 * rank), bf16),
            pltpu.VMEM((count, rows, depth), bf16),
            pltpu.VMEM((count, rows, depth), bf16),
            pltpu.VMEM((rows, depth), bf16),
            pltpu.VMEM((count, 2 * rank, depth), bf16),
            pltpu.VMEM((landing, 2 * rank, depth), bf16),
            pltpu.VMEM((2 * rank, rows), f32),
            pltpu.VMEM((count, 2 * rank, rows), bf16),
            pltpu.VMEM((count, 2, tokens, heads), bf16),
            pltpu.VMEM((max(count - 2, 1), 2, tokens, heads), bf16),
            pltpu.SemaphoreType.DMA((copies,)),
            pltpu.SemaphoreType.DMA((copies,)),
            pltpu.SemaphoreType.DMA((11,)),
        ],
        compiler_params=pltpu.CompilerParams(
            has_side_effects=True, collective_id=0, vmem_limit_bytes=kernel_mib * 2**20
        ),
        cost_estimate=pl.CostEstimate(
            flops=8 * tokens * depth * wide, bytes_accessed=4 * depth * wide, transcendentals=0
        ),
        name="layer",
    )(gain, arr, kept, ret, wk, wv, dnk, dnv, upk, upv, ck, cv)


def store_kernel(cuts, own, got, inv, grad, dgk, dgv, ugk, ugv, *refs):
    outs, (keys_v, values_v, sem) = refs[:7], refs[7:]
    copies = []

    def store(src, dst):
        copies.append(pltpu.make_async_copy(src, dst, sem.at[len(copies)]))
        copies[-1].start()

    step = grad.shape[0] // cuts
    for i in range(cuts):
        at = pl.ds(i * step, step)
        store(grad.at[at], outs[2].at[at])
    for src, dst in zip((dgk, dgv, ugk, ugv), outs[3:]):
        store(src, dst)
    for r, head in enumerate((keys_v, values_v)):

        cut = min(store_tile, head.shape[0])
        for i in range(0, head.shape[0], cut):
            at = slice(i, i + cut)
            total = own[r, at, :].astype(f32) + got[r, at, :].astype(f32)
            head[at, :] = (inv[at, :1] * total).astype(bf16)
        store(head, outs[r])
    for copy in copies:
        copy.wait()


def store(results):
    own, _, _, *rest = results
    head = jax.ShapeDtypeStruct(own.shape[1:], bf16)
    cuts = 4
    return pl.pallas_call(
        functools.partial(store_kernel, cuts),
        in_specs=[pl.BlockSpec(memory_space=pltpu.VMEM)] * len(results),
        out_specs=[pl.BlockSpec(memory_space=pl.ANY)] * 7,
        out_shape=[head, head] + [jax.ShapeDtypeStruct(x.shape, x.dtype) for x in rest],
        scratch_shapes=[pltpu.VMEM(head.shape, bf16)] * 2
        + [pltpu.SemaphoreType.DMA((cuts + 6,))],
        compiler_params=pltpu.CompilerParams(vmem_limit_bytes=store_mib * 2**20),
        name="store",
    )(*results)


def on_device(
    arriving,
    kept_input,
    returning,
    norm_gain,
    key_weight,
    value_weight,
    key_down,
    value_down,
    key_up,
    value_up,
    key_cot,
    value_cot,
):
    keys, values, input_grad, dgk, dgv, ugk, ugv = store(run_layer(
        lax.axis_size("tensor"),
        lax.axis_size("section"),
        arriving[0],
        kept_input[0],
        returning[0],
        norm_gain,
        key_weight[0],
        value_weight[0],
        key_down[0].T,
        value_down[0].T,
        key_up[0],
        value_up[0],
        key_cot[0],
        value_cot[0],
    ))
    return (
        keys[None],
        values[None],
        input_grad[None],
        dgk.T[None],
        dgv.T[None],
        ugk[None],
        ugv[None],
    )


def solution(mesh):
    return jax.shard_map(
        on_device,
        mesh=mesh,
        in_specs=(
            P("section", "tensor", None),
            P("section", "tensor", None),
            P("section", "tensor", None),
            P("section", None),
            P("section", "tensor", None),
            P("section", "tensor", None),
            P("section", "tensor", None),
            P("section", "tensor", None),
            P("section", None, "tensor"),
            P("section", None, "tensor"),
            P("section", None, "tensor"),
            P("section", None, "tensor"),
        ),
        out_specs=(
            P("section", None, "tensor"),
            P("section", None, "tensor"),
            P("section", "tensor", None),
            P("section", "tensor", None),
            P("section", "tensor", None),
            P("section", None, "tensor"),
            P("section", None, "tensor"),
        ),
        check_vma=False,
    )
```

```python
import functools

import jax
import jax.numpy as jnp
from jax import lax
from jax.experimental import pallas as pl
from jax.experimental.pallas import tpu as pltpu
from jax.sharding import PartitionSpec as P

epsilon = 1e-05
adapter_scale = 2.0
bf16 = jnp.bfloat16
f32 = jnp.float32
MESH = pl.DeviceIdType.MESH
lanes = 128
cuts_of_16 = (0, 4, 8, 12, 14, 16)
parts = len(cuts_of_16) - 1
halves = 2
row_tile = 16
kernel_mib = 55
store_mib = 16
store_tile = 128


def flip(z, mask):
    bit = 1
    while bit <= mask:
        if mask & bit:
            z = z + bit - 2 * bit * ((z // bit) % 2)
        bit *= 2
    return z


def bits_up(count):
    bits = []
    bit = 1
    while bit < count:
        bits.append(bit)
        bit *= 2
    return bits


def dot_nt(a, b):
    return lax.dot_general(a, b, (((1,), (1,)), ((), ())), preferred_element_type=f32)


def dot_nn(a, b):
    return jnp.dot(a, b, preferred_element_type=f32)


def layer_kernel(
    count,
    sections,
    gain,
    arr,
    kept,
    ret,
    wk,
    wv,
    dnk,
    dnv,
    upk,
    upv,
    ck,
    cv,
    own_out,
    sum_out,
    inv_f,
    grad_out,
    dgk_out,
    dgv_out,
    ugk_out,
    ugv_out,
    gain_ref,
    wk_v,
    wv_v,
    cotk,
    cotv,
    upk_v,
    upv_v,
    dn_v,
    arr_v,
    kept_v,
    back_v,
    x_v,
    inv_t,
    inv_in,
    inv_b,
    ad_v,
    adt_v,
    mid_v,
    bo_v,
    bi_v,
    nb_v,
    dp_v,
    dp_in,
    km_sum,
    km_v,
    sums_v,
    sums_in,
    send_sem,
    recv_sem,
    local_sem,
):
    rows, width = kept.shape
    depth = wk.shape[0]
    tokens, heads = ck.shape
    rank = upk.shape[0]
    s = lax.axis_index("section")
    z = lax.axis_index("tensor")
    ahead = lax.rem(s + 1, sections)
    behind = lax.rem(s + sections - 1, sections)
    used = [0, 0]

    def load(src, dst):
        copy = pltpu.make_async_copy(src, dst, local_sem.at[used[1]])
        used[1] += 1
        copy.start()
        return copy

    sent = []

    def remote(src, dst, k, section, tensor):
        return pltpu.make_async_remote_copy(
            src_ref=src,
            dst_ref=dst,
            send_sem=send_sem.at[k],
            recv_sem=recv_sem.at[k],
            device_id=(section, tensor),
            device_id_type=MESH,
        )

    def later(src, dst, section, tensor):
        copy = remote(src, dst, used[0], section, tensor)
        used[0] += 1
        sent.append(copy)
        return copy

    def send(src, dst, section, tensor):
        copy = later(src, dst, section, tensor)
        copy.start()
        return copy

    def head_cols(q):
        return pl.ds(pl.multiple_of(q * heads, heads), heads)

    def depth_cols(q):
        return pl.ds(pl.multiple_of(q * depth, depth), depth)

    greet = [(behind, flip(z, j)) for j in reversed(range(count))]
    greet += [(s, flip(z, j)) for j in reversed(range(1, count))] + [(ahead, z)]
    entry = pltpu.get_barrier_semaphore()
    for peer in greet:
        pl.semaphore_signal(entry, inc=1, device_id=peer, device_id_type=MESH)

    bits = bits_up(count)
    own = [
        load(ck, cotk.at[:, head_cols(z)]),
        load(cv, cotv.at[:, head_cols(z)]),
        load(upk, upk_v.at[:, head_cols(z)]),
        load(upv, upv_v.at[:, head_cols(z)]),
    ]
    own_down = [load(dnk, dn_v.at[z, :rank]), load(dnv, dn_v.at[z, rank:])]
    arr_load = load(arr, arr_v)
    kept_load = load(kept, kept_v)
    weights = [load(gain, gain_ref), load(wk, wk_v), load(wv, wv_v)]
    for copy in own + own_down:
        copy.wait()
    pl.semaphore_wait(entry, len(greet))

    def inside(q):
        return (q >= 0) & (q < count)

    head_kinds = (cotk, cotv, upk_v, upv_v)
    guarded = []

    def relay(step, kinds):
        landing = []
        for way in (1, -1):
            q, to, come = z - way * (step - 1), z + way, z - way * step
            going = inside(q) & inside(to)
            for kind in kinds:
                if kind == 4:
                    block, got = dn_v.at[q], dn_v.at[come]
                else:
                    buf = head_kinds[kind]
                    block, got = buf.at[:, head_cols(q)], buf.at[:, head_cols(come)]
                k = used[0]
                used[0] += 1
                out = remote(block, block, k, s, to)
                pl.when(going)(out.start)
                guarded.append((going, out))
                landing.append((kind, inside(come), remote(got, got, k, s, z)))
        return landing

    def landed(landing, kinds):
        for kind, coming, copy in landing:
            if kind in kinds:
                pl.when(coming)(copy.wait_recv)

    half = rows // halves
    ends = (z == 0) | (z == count - 1)

    def arriving(j, i):
        q = flip(z, j)
        at = pl.ds(i * half, half)
        return later(arr.at[at, depth_cols(q)], x_v.at[z, at], ahead, q)

    far = list(range(max(bits[-1], 1), count)) if bits else []
    near = [j for j in range(1, count) if j not in far]
    arrivals = {(j, i): arriving(j, i) for j in range(count) for i in range(halves)}

    def start_near():
        for i in range(halves):
            for j in near:
                arrivals[j, i].start()

    def start_far(i):
        for j in far:
            arrivals[j, i].start()

    heads_only, down_only = (0, 1, 2, 3), (4,)
    landing = relay(1, heads_only) if bits else []
    for i in range(halves):
        arrivals[0, i].start()
    returned = send(ret, back_v, behind, z)
    landing += relay(1, down_only) if bits else []
    pl.when(ends)(start_near)

    arr_load.wait()

    def arr_stats(i, _):
        at = pl.ds(pl.multiple_of(i * row_tile, row_tile), row_tile)
        x = arr_v[at, :].astype(f32)
        inverse = lax.rsqrt(jnp.mean(x * x, axis=-1, keepdims=True) + epsilon)
        inv_t[at, :] = jnp.broadcast_to(inverse, (row_tile, lanes))
        return 0

    lax.fori_loop(0, rows // row_tile, arr_stats, 0)
    inv_in[z] = inv_t[...].T[:8]
    inverses = [
        send(inv_in.at[z, :1], inv_in.at[z + count, :1], ahead, flip(z, j)) for j in range(count)
    ]
    kept_load.wait()

    def kept_stats(i, _):
        at = pl.ds(pl.multiple_of(i * row_tile, row_tile), row_tile)
        x = kept_v[at, :].astype(f32)
        inverse = lax.rsqrt(jnp.mean(x * x, axis=-1, keepdims=True) + epsilon)
        inv_b[at, :] = jnp.broadcast_to(inverse, (row_tile, lanes))
        return 0

    for step in range(1, count):
        landed(landing, heads_only)
        ahead_of = relay(step + 1, heads_only) if step + 1 < count else []
        landed(landing, down_only)
        ahead_of += relay(step + 1, down_only) if step + 1 < count else []
        landing = ahead_of
        if step <= halves:
            start_far(step - 1)
        if step == 1:
            lax.fori_loop(0, rows // row_tile, kept_stats, 0)
        if step == max(count - 2, 1):
            pl.when(jnp.logical_not(ends))(start_near)
    for i in range(max(count - 1, 0), halves):
        start_far(i)
    if count == 1:
        lax.fori_loop(0, rows // row_tile, kept_stats, 0)
    for copy in weights:
        copy.wait()

    for r, (cot, up) in enumerate(((cotk, upk_v), (cotv, upv_v))):
        ad_v[:, r * rank : (r + 1) * rank] = adapter_scale * dot_nt(cot[...], up[...])
        adt_v[r * rank : (r + 1) * rank, :] = adapter_scale * dot_nt(up[...], cot[...])

    tile = min(512, depth)

    def branch_tile(i, _):
        at = pl.ds(pl.multiple_of(i * tile, tile), tile)
        total = dot_nn(ad_v[...].astype(bf16), dn_v[z, :, at])
        total = total + dot_nt(cotk[...], wk_v[at, :])
        total = total + dot_nt(cotv[...], wv_v[at, :])
        bo_v[:, :, at] = total.astype(bf16).reshape(count, rows, tile)
        return 0

    lax.fori_loop(0, depth // tile, branch_tile, 0)
    cuts = [rows * cut // 16 for cut in cuts_of_16]
    others = far + near

    def branch(j, i):
        at = pl.ds(cuts[i], cuts[i + 1] - cuts[i])
        q = flip(z, j)
        return later(bo_v.at[q, at], bi_v.at[z, at], s, q)

    branches = {(j, i): branch(j, i) for j in others for i in range(parts)}

    held_back = (count - 1, parts - 1)

    def send_branches(group):
        for i in range(1, parts):
            for j in group:
                if group is others or (j, i) != held_back:
                    branches[j, i].start()

    for j in others:
        branches[j, 0].start()
    pl.when(jnp.logical_not(ends))(functools.partial(send_branches, far))

    def own_branch(i, _):
        at = pl.ds(pl.multiple_of(i * row_tile, row_tile), row_tile)
        bi_v[z, at, :] = bo_v[z, at, :]
        return 0

    lax.fori_loop(0, rows // row_tile, own_branch, 0)

    mine = adt_v[:, pl.ds(pl.multiple_of(z * rows, rows), rows)].astype(bf16)

    km_sum[...] = jnp.zeros((2 * rank, rows), f32)

    def kept_block(j, _):
        inverse = inv_b[:, :1]

        def normalize(i, _):
            at = pl.ds(pl.multiple_of(i * tile, tile), tile)
            cols = pl.ds(pl.multiple_of(j * depth + i * tile, tile), tile)
            part = kept_v[:, cols].astype(f32) * inverse * gain_ref[:, cols].astype(f32)
            nb_v[:, at] = part.astype(bf16)
            return 0

        lax.fori_loop(0, depth // tile, normalize, 0)
        km_sum[...] += dot_nt(dn_v[j], nb_v[...])
        dp_v[j] = dot_nn(mine, nb_v[...]).astype(bf16)
        return 0

    lax.fori_loop(0, count, kept_block, 0)
    km_v[z] = (adapter_scale * km_sum[...]).astype(bf16)
    mids = [send(km_v.at[z], km_v.at[z], s, flip(z, j)) for j in range(1, count)]

    def down_slot(k):
        return dp_in.at[k]

    def sum_slot(k):
        return sum_out if k == count - 2 else sums_in.at[k]

    def scatter_stage(buf, landing, bit):
        to = flip(z, bit)
        offset = sum(count // (2 * b) for b in bits if b < bit)
        return [
            send(buf.at[flip(z, bit ^ m)], landing(offset + k), s, to)
            for k, m in enumerate(range(0, count, 2 * bit))
        ]

    def scatter_add(buf, landing, bit, copies):
        offset = sum(count // (2 * b) for b in bits if b < bit)
        for k, m in enumerate(range(0, count, 2 * bit)):
            copies[k].wait_recv()
            q = flip(z, m)
            buf[q] = (buf[q].astype(f32) + landing(offset + k)[...].astype(f32)).astype(bf16)

    down_stage = scatter_stage(dp_v, down_slot, bits[0]) if bits else []

    def head_block(q):
        gain_cols = depth_cols(z)

        def scale(i, _):
            at = pl.ds(pl.multiple_of(i * row_tile, row_tile), row_tile)
            x_v[q, at, :] = (x_v[q, at, :].astype(f32) * gain_ref[:, gain_cols].astype(f32)).astype(bf16)
            return 0

        lax.fori_loop(0, rows // row_tile, scale, 0)
        mid = adapter_scale * dot_nt(x_v[q], dn_v[z])
        mid_v[...] = mid.astype(bf16)
        at = pl.ds(pl.multiple_of(q * rows, rows), rows)

        def head_cut(d, _):
            cols = head_cols(d)
            for r, (w, up) in enumerate(((wk_v, upk_v), (wv_v, upv_v))):
                total = dot_nn(x_v[q], w[:, cols])
                total = total + dot_nn(mid_v[:, r * rank : (r + 1) * rank], up[:, cols])
                sums_v[d, r, at, :] = total.astype(bf16)
            return 0

        lax.fori_loop(0, count, head_cut, 0)

    for j in [0] + far + near:
        for i in range(halves):
            arrivals[j, i].wait_recv()
        head_block(flip(z, j))
    for k, bit in enumerate(bits):
        stage = scatter_stage(sums_v, sum_slot, bit)
        if k == 0:
            pl.when(ends)(functools.partial(send_branches, others))
            pl.when(jnp.logical_not(ends))(functools.partial(send_branches, near))
        if k + 1 < len(bits):
            scatter_add(dp_v, down_slot, bit, down_stage)
            down_stage = scatter_stage(dp_v, down_slot, bits[k + 1])
            scatter_add(sums_v, sum_slot, bit, stage)

    if others:
        pl.when(jnp.logical_not(ends))(branches[held_back].start)
    for copy in mids:
        copy.wait_recv()
    for r, cot in enumerate((cotk, cotv)):
        total = jnp.zeros((rank, heads), f32)
        for q in range(count):
            mid = km_v[q, r * rank : (r + 1) * rank, :]
            total = total + dot_nn(mid, cot[q * rows : (q + 1) * rows, head_cols(z)])
        (ugk_out, ugv_out)[r][...] = total
    for copy in inverses:
        copy.wait_recv()
    for q in range(count):
        spread = jnp.broadcast_to(inv_in[count + q, :1, :], (lanes, rows)).T
        inv_f[q * rows : (q + 1) * rows, :] = spread
    own_out[...] = sums_v[z]
    returned.wait_recv()

    def grad_tile(i, _):
        at = pl.ds(pl.multiple_of(i * row_tile, row_tile), row_tile)
        inverse = inv_b[at, :1]
        inner = jnp.zeros((row_tile, 1), f32)
        for j in range(count):
            cols = slice(j * depth, (j + 1) * depth)
            scaled = gain_ref[:, cols].astype(f32) * bi_v[j, at, :].astype(f32)
            inner = inner + jnp.sum(kept_v[at, cols].astype(f32) * scaled, axis=-1, keepdims=True)
        pull = inverse * inverse * inverse * (inner / width)
        for j in range(count):
            cols = slice(j * depth, (j + 1) * depth)
            scaled = gain_ref[:, cols].astype(f32) * bi_v[j, at, :].astype(f32)
            value = back_v[at, cols].astype(f32) + inverse * scaled - kept_v[at, cols].astype(f32) * pull
            grad_out[at, cols] = value.astype(bf16)
        return 0

    def finish(i):
        for j in others:
            branches[j, i].wait_recv()
        lax.fori_loop(cuts[i] // row_tile, cuts[i + 1] // row_tile, grad_tile, 0)

    for i in range(parts - 1):
        finish(i)
    if bits:
        scatter_add(dp_v, down_slot, bits[-1], down_stage)
    dgk_out[...] = dp_v[z, :rank].astype(f32)
    dgv_out[...] = dp_v[z, rank:].astype(f32)
    finish(parts - 1)
    if bits:
        stage[0].wait_recv()
    else:
        sum_out[...] = jnp.zeros(sum_out.shape, bf16)
    for copy in sent:
        copy.wait_send()
    for going, copy in guarded:
        pl.when(going)(copy.wait_send)


def run_layer(count, sections, arr, kept, ret, gain, wk, wv, dnk, dnv, upk, upv, ck, cv):
    rows, width = kept.shape
    depth, wide = wk.shape
    tokens, heads = ck.shape
    rank = upk.shape[0]
    copies = 10 * (count - 1) + halves * count + count + 1
    copies += parts * (count - 1) + 3 * (count - 1)
    hbm = pl.BlockSpec(memory_space=pl.ANY)
    landing = max(count - 1, 1)
    return pl.pallas_call(
        functools.partial(layer_kernel, count, sections),
        in_specs=[hbm] * 12,
        out_specs=[pl.BlockSpec(memory_space=pltpu.VMEM)] * 8,
        out_shape=[
            pltpu.VMEM((2, tokens, heads), bf16),
            pltpu.VMEM((2, tokens, heads), bf16),
            pltpu.VMEM((tokens, lanes), f32),
            pltpu.VMEM((rows, width), bf16),
            pltpu.VMEM((rank, depth), f32),
            pltpu.VMEM((rank, depth), f32),
            pltpu.VMEM((rank, heads), f32),
            pltpu.VMEM((rank, heads), f32),
        ],
        scratch_shapes=[
            pltpu.VMEM((1, width), bf16),
            pltpu.VMEM((depth, wide), bf16),
            pltpu.VMEM((depth, wide), bf16),
            pltpu.VMEM((tokens, wide), bf16),
            pltpu.VMEM((tokens, wide), bf16),
            pltpu.VMEM((rank, wide), bf16),
            pltpu.VMEM((rank, wide), bf16),
            pltpu.VMEM((count, 2 * rank, depth), bf16),
            pltpu.VMEM((rows, width), bf16),
            pltpu.VMEM((rows, width), bf16),
            pltpu.VMEM((rows, width), bf16),
            pltpu.VMEM((count, rows, depth), bf16),
            pltpu.VMEM((rows, lanes), f32),
            pltpu.VMEM((2 * count, 8, rows), f32),
            pltpu.VMEM((rows, lanes), f32),
            pltpu.VMEM((tokens, 2 * rank), f32),
            pltpu.VMEM((2 * rank, tokens), f32),
            pltpu.VMEM((rows, 2 * rank), bf16),
            pltpu.VMEM((count, rows, depth), bf16),
            pltpu.VMEM((count, rows, depth), bf16),
            pltpu.VMEM((rows, depth), bf16),
            pltpu.VMEM((count, 2 * rank, depth), bf16),
            pltpu.VMEM((landing, 2 * rank, depth), bf16),
            pltpu.VMEM((2 * rank, rows), f32),
            pltpu.VMEM((count, 2 * rank, rows), bf16),
            pltpu.VMEM((count, 2, tokens, heads), bf16),
            pltpu.VMEM((max(count - 2, 1), 2, tokens, heads), bf16),
            pltpu.SemaphoreType.DMA((copies,)),
            pltpu.SemaphoreType.DMA((copies,)),
            pltpu.SemaphoreType.DMA((11,)),
        ],
        compiler_params=pltpu.CompilerParams(
            has_side_effects=True, collective_id=0, vmem_limit_bytes=kernel_mib * 2**20
        ),
        cost_estimate=pl.CostEstimate(
            flops=8 * tokens * depth * wide, bytes_accessed=4 * depth * wide, transcendentals=0
        ),
        name="layer",
    )(gain, arr, kept, ret, wk, wv, dnk, dnv, upk, upv, ck, cv)


def store_kernel(cuts, own, got, inv, grad, dgk, dgv, ugk, ugv, *refs):
    outs, (keys_v, values_v, sem) = refs[:7], refs[7:]
    copies = []

    def store(src, dst):
        copies.append(pltpu.make_async_copy(src, dst, sem.at[len(copies)]))
        copies[-1].start()

    step = grad.shape[0] // cuts
    for i in range(cuts):
        at = pl.ds(i * step, step)
        store(grad.at[at], outs[2].at[at])
    for src, dst in zip((dgk, dgv, ugk, ugv), outs[3:]):
        store(src, dst)
    for r, head in enumerate((keys_v, values_v)):

        cut = min(store_tile, head.shape[0])
        for i in range(0, head.shape[0], cut):
            at = slice(i, i + cut)
            total = own[r, at, :].astype(f32) + got[r, at, :].astype(f32)
            head[at, :] = (inv[at, :1] * total).astype(bf16)
        store(head, outs[r])
    for copy in copies:
        copy.wait()


def store(results):
    own, _, _, *rest = results
    head = jax.ShapeDtypeStruct(own.shape[1:], bf16)
    cuts = 4
    return pl.pallas_call(
        functools.partial(store_kernel, cuts),
        in_specs=[pl.BlockSpec(memory_space=pltpu.VMEM)] * len(results),
        out_specs=[pl.BlockSpec(memory_space=pl.ANY)] * 7,
        out_shape=[head, head] + [jax.ShapeDtypeStruct(x.shape, x.dtype) for x in rest],
        scratch_shapes=[pltpu.VMEM(head.shape, bf16)] * 2
        + [pltpu.SemaphoreType.DMA((cuts + 6,))],
        compiler_params=pltpu.CompilerParams(vmem_limit_bytes=store_mib * 2**20),
        name="store",
    )(*results)


def on_device(
    arriving,
    kept_input,
    returning,
    norm_gain,
    key_weight,
    value_weight,
    key_down,
    value_down,
    key_up,
    value_up,
    key_cot,
    value_cot,
):
    keys, values, input_grad, dgk, dgv, ugk, ugv = store(run_layer(
        lax.axis_size("tensor"),
        lax.axis_size("section"),
        arriving[0],
        kept_input[0],
        returning[0],
        norm_gain,
        key_weight[0],
        value_weight[0],
        key_down[0].T,
        value_down[0].T,
        key_up[0],
        value_up[0],
        key_cot[0],
        value_cot[0],
    ))
    return (
        keys[None],
        values[None],
        input_grad[None],
        dgk.T[None],
        dgv.T[None],
        ugk[None],
        ugv[None],
    )


def solution(mesh):
    return jax.shard_map(
        on_device,
        mesh=mesh,
        in_specs=(
            P("section", "tensor", None),
            P("section", "tensor", None),
            P("section", "tensor", None),
            P("section", None),
            P("section", "tensor", None),
            P("section", "tensor", None),
            P("section", "tensor", None),
            P("section", "tensor", None),
            P("section", None, "tensor"),
            P("section", None, "tensor"),
            P("section", None, "tensor"),
            P("section", None, "tensor"),
        ),
        out_specs=(
            P("section", None, "tensor"),
            P("section", None, "tensor"),
            P("section", "tensor", None),
            P("section", "tensor", None),
            P("section", "tensor", None),
            P("section", None, "tensor"),
            P("section", None, "tensor"),
        ),
        check_vma=False,
    )
```
